32 devices in a mesh: img: 8 (over z, core), txt: 4 (over y, x).
Axes of the slice: x: 2, y: 2, z: 4, core: 2. Of those that a mesh axis runs over, the one named last changes fastest.
Arguments:
- teacher_img: bfloat16 [8192, 1280], P('img'), may hold values from -40 to 40
- teacher_txt: bfloat16 [4096, 1280], P('txt'), may hold values from -40 to 40
- student_img: bfloat16 [8192, 512], P('img'), may hold values from -40 to 40
- student_txt: bfloat16 [4096, 512], P('txt'), may hold values from -40 to 40
Outputs:
- loss: float32 [], replicated
- grad_img: float32 [8192, 512], P(('img', 'txt'))
- grad_txt: float32 [4096, 512], P(('txt', 'img'))
The draws below stay inside these ranges and needn't reach their ends.
All inputs are finite; a program needn't handle non-finite values.
Results may differ from the reference program's by a relative error of at most 0.0033.
Values sent between devices are 32-bit elements; how exact they have to be, the bound alone decides.
A program may use at most 64 MiB of HBM per device.

```python
import math
import jax
import jax.numpy as jnp
from jax import lax

DT = 1280
DS = 512
ROWS = 1024
IMAGES = 8192
TEXTS = 4096


def embed_pair(key, width, marker):
    base = jax.random.fold_in(key, marker)
    keys = jax.random.split(base, 2)
    images = jnp.clip(jax.random.normal(keys[0], (IMAGES, width), jnp.float32), -5.0, 5.0)
    texts = jnp.clip(jax.random.normal(keys[1], (TEXTS, width), jnp.float32), -5.0, 5.0)
    return (images.astype(jnp.bfloat16), texts.astype(jnp.bfloat16))


def draw_teacher_img(key, part):
    return embed_pair(key, DT, 11)[0]


def draw_teacher_txt(key, part):
    return embed_pair(key, DT, 11)[1]


def draw_student_img(key, part):
    return embed_pair(key, DS, 23)[0]


def draw_student_txt(key, part):
    return embed_pair(key, DS, 23)[1]


def setup_inputs(seed: int = 0) -> dict:
    streams_of = jax.random.split(jax.random.key(seed), 5)
    return {
        "teacher_img": draw_teacher_img(jax.random.fold_in(streams_of[4], 71), 0),
        "teacher_txt": draw_teacher_txt(jax.random.fold_in(streams_of[4], 71), 0),
        "student_img": draw_student_img(jax.random.fold_in(streams_of[4], 71), 0),
        "student_txt": draw_student_txt(jax.random.fold_in(streams_of[4], 71), 0),
    }


def logits(left, right, width):
    return 3.0 / math.sqrt(width) * jnp.dot(left, right.T, preferred_element_type=jnp.float32)

def join_pair(peak_one, mass_one, peak_two, mass_two):
    highest = jnp.maximum(peak_one, peak_two)
    return (highest, mass_one * jnp.exp(peak_one - highest) + mass_two * jnp.exp(peak_two - highest))

def reference(teacher_img, teacher_txt, student_img, student_txt):
    blocks = IMAGES // ROWS
    scale_learn = 3.0 / math.sqrt(DS)
    teach_rows = teacher_img.reshape(blocks, ROWS, DT)
    learn_rows = student_img.reshape(blocks, ROWS, DS)

    def first_pass(carry, pieces):
        teach_peak, teach_mass, learn_peak, learn_mass = carry
        teach_block = logits(pieces[0], teacher_txt, DT)
        learn_block = logits(pieces[1], student_txt, DS)
        row_teach = jax.scipy.special.logsumexp(teach_block, axis=1)
        row_learn = jax.scipy.special.logsumexp(learn_block, axis=1)
        block_peak = lax.optimization_barrier(jnp.max(teach_block, axis=0))
        block_mass = lax.optimization_barrier(jnp.sum(jnp.exp(teach_block - block_peak[None, :]), axis=0))
        teach_peak, teach_mass = join_pair(teach_peak, teach_mass, block_peak, block_mass)
        block_peak = lax.optimization_barrier(jnp.max(learn_block, axis=0))
        block_mass = lax.optimization_barrier(jnp.sum(jnp.exp(learn_block - block_peak[None, :]), axis=0))
        learn_peak, learn_mass = join_pair(learn_peak, learn_mass, block_peak, block_mass)
        return ((teach_peak, teach_mass, learn_peak, learn_mass), (row_teach, row_learn))
    lowest = jnp.full((TEXTS,), -jnp.inf, jnp.float32)
    nothing = jnp.zeros((TEXTS,), jnp.float32)
    carry, (row_teach, row_learn) = lax.scan(first_pass, (lowest, nothing, lowest, nothing), (teach_rows, learn_rows))
    col_teach = carry[0] + jnp.log(carry[1])
    col_learn = carry[2] + jnp.log(carry[3])

    def second_pass(carry, pieces):
        grad_text, row_total, col_total = carry
        teach_part, learn_part, teach_norm, learn_norm = pieces
        teach_block = logits(teach_part, teacher_txt, DT)
        learn_block = logits(learn_part, student_txt, DS)
        p_row = jnp.exp(teach_block - teach_norm[:, None])
        q_row = jnp.exp(learn_block - learn_norm[:, None])
        p_col = jnp.exp(teach_block - col_teach[None, :])
        q_col = jnp.exp(learn_block - col_learn[None, :])
        gap = teach_block - learn_block
        row_total = row_total + jnp.sum(p_row * gap) + jnp.sum(learn_norm - teach_norm)
        col_total = col_total + jnp.sum(p_col * gap)
        delta = (8.0 * (q_row - p_row + q_col - p_col)).astype(jnp.bfloat16)
        grad_block = scale_learn * jnp.dot(delta, student_txt, preferred_element_type=jnp.float32)
        grad_text = grad_text + scale_learn * jnp.dot(delta.T, learn_part, preferred_element_type=jnp.float32)
        return ((grad_text, row_total, col_total), grad_block)
    start = (jnp.zeros((TEXTS, DS), jnp.float32), jnp.zeros((), jnp.float32), jnp.zeros((), jnp.float32))
    (grad_txt, row_total, col_total), grad_blocks = lax.scan(second_pass, start, (teach_rows, learn_rows, row_teach, row_learn))
    col_total = col_total + jnp.sum(col_learn - col_teach)
    loss = 0.5 * (row_total / IMAGES + col_total / TEXTS)
    grad_img = grad_blocks.reshape(IMAGES, DS)
    return (loss, grad_img, grad_txt)
```

```python
import functools
import math

import jax
import jax.numpy as jnp
from jax import lax
from jax.experimental import pallas as pl
from jax.experimental.pallas import tpu as pltpu
from jax.sharding import PartitionSpec as P

LANES = 128
LOG2E = math.log2(math.e)
LN2 = math.log(2.0)
MESH = pl.DeviceIdType.MESH
F32 = jnp.float32
NT = (((1,), (1,)), ((), ()))


def minor_of(n):
    return 1 << ((n.bit_length() - 1) // 2)


def kernel(
    img_n, txt_n,
    timg_hbm, ttxt_hbm, simg_hbm, stxt_hbm,
    loss_ref, gimg_ref, gtxt_ref,
    timg, ttxt, simg, stxt, t2, s2, q, row_at, cstat, rslot, cslot, delta, deltat,
    gi, g1a, g1b, g2a, g2b, gt, xr, zr, lrow, lcol,
    in_sem, rs_send, rs_recv, cs_send, cs_recv, a1_send, a1_recv, b1_send, b1_recv,
    a2_send, a2_recv, b2_send, b2_recv, x_send, x_recv,
    z_send, z_recv, l1_send, l1_recv, l2_send, l2_recv,
):
    rows, wide = timg.shape
    cols, deep = stxt.shape
    strips = rows // LANES
    pieces = cols // LANES
    mi = lax.axis_index("img")
    mt = lax.axis_index("txt")
    levels = img_n // 2
    mz = mi // 2
    mc = lax.rem(mi, 2)
    scale_t = 3.0 / math.sqrt(wide) * LOG2E
    scale_s = 3.0 / math.sqrt(deep) * LOG2E
    scale_g = 3.0 / math.sqrt(deep)

    loads = [
        pltpu.make_async_copy(src, dst, in_sem.at[k])
        for k, (src, dst) in enumerate(
            ((simg_hbm, simg), (stxt_hbm, stxt), (timg_hbm, timg), (ttxt_hbm, ttxt))
        )
    ]
    for load in loads:
        load.start()

    barrier = pltpu.get_barrier_semaphore()
    txt_peers = [lax.rem(mt + d, txt_n) for d in range(1, txt_n)]
    img_peers = [lax.rem(mi + d, img_n) for d in range(1, img_n)]
    for p in txt_peers:
        pl.semaphore_signal(barrier, inc=1, device_id=(mi, p), device_id_type=MESH)
    for p in img_peers:
        pl.semaphore_signal(barrier, inc=1, device_id=(p, mt), device_id_type=MESH)

    def to_txt(src, dst, send, recv, p):
        return pltpu.make_async_remote_copy(
            src_ref=src, dst_ref=dst, send_sem=send, recv_sem=recv,
            device_id=(mi, p), device_id_type=MESH,
        )

    def to_img(src, dst, send, recv, p):
        return pltpu.make_async_remote_copy(
            src_ref=src, dst_ref=dst, send_sem=send, recv_sem=recv,
            device_id=(p, mt), device_id_type=MESH,
        )

    lane = lax.broadcasted_iota(jnp.int32, (8, LANES), 1)

    chunk = min(2 * LANES, cols)
    stat_out = []

    def product(left, right, out, factor, slot):
        def one(j, c):
            at = pl.ds(pl.multiple_of(j * chunk, chunk), chunk)
            tile = factor * lax.dot_general(
                left[...], right[at, :], NT, preferred_element_type=F32
            )
            out[:, at] = tile
            cstat[slot, 0:1, at] = jnp.max(tile, axis=0, keepdims=True)
            return c

        lax.fori_loop(0, cols // chunk, one, 0)

    def masses(out, slot):
        def group(g, mass):
            here = pl.ds(pl.multiple_of(g * 8, 8), 8)
            x = out[here, :]
            peak = jnp.max(x, axis=1, keepdims=True)
            row = jnp.sum(jnp.exp2(x - peak), axis=1, keepdims=True)
            row_at[slot, here, :] = jnp.where(lane == 0, peak, row)
            return mass + jnp.exp2(x - cstat[slot, 0:1, :])

        mass = lax.fori_loop(0, rows // 8, group, jnp.zeros((8, cols), F32), unroll=8)
        tops = cstat[slot, 0:1, :]
        sums = jnp.sum(mass, axis=0, keepdims=True)
        for k in range(pieces):
            at = slice(k * LANES, (k + 1) * LANES)
            cslot[slot, mi, 0, k : k + 1, :] = tops[:, at]
            cslot[slot, mi, 1, k : k + 1, :] = sums[:, at]
        for k in range(strips):
            turned = row_at[slot, k * LANES : (k + 1) * LANES, :].T
            rslot[slot, mt, 0, k : k + 1, :] = turned[0:1, :]
            rslot[slot, mt, 1, k : k + 1, :] = turned[1:2, :]
        if slot == 1:
            pl.semaphore_wait(barrier, txt_n - 1 + img_n - 1)
        copies = [
            to_img(
                cslot.at[slot, mi], cslot.at[slot, mi],
                cs_send.at[slot, d], cs_recv.at[slot, mi], p,
            )
            for d, p in reversed(list(enumerate(img_peers)))
        ] + [
            to_txt(
                rslot.at[slot, mt], rslot.at[slot, mt],
                rs_send.at[slot, d], rs_recv.at[slot, mt], p,
            )
            for d, p in enumerate(txt_peers)
        ]
        for copy in copies:
            copy.start()
        stat_out.extend(copies)

    loads[0].wait()
    loads[1].wait()
    product(simg, stxt, s2, scale_s, 1)
    masses(s2, 1)
    loads[2].wait()
    loads[3].wait()
    product(timg, ttxt, t2, scale_t, 0)
    masses(t2, 0)

    def joined(slot, n):
        peaks = [slot[k, 0] for k in range(n)]
        top = functools.reduce(jnp.maximum, peaks)
        mass = functools.reduce(
            jnp.add, [slot[k, 1] * jnp.exp2(peaks[k] - top) for k in range(n)]
        )
        return top + jnp.log(mass) * LOG2E

    def gathered(slot):
        for d, p in enumerate(txt_peers):
            to_txt(
                rslot.at[slot, p], rslot.at[slot, p],
                rs_send.at[slot, d], rs_recv.at[slot, p], p,
            ).wait_recv()
        row = joined(rslot.at[slot], txt_n)
        for k in range(strips):
            row_at[slot, k * LANES : (k + 1) * LANES, :] = jnp.broadcast_to(
                row[k : k + 1], (LANES, LANES)
            ).T
        for d, p in enumerate(img_peers):
            to_img(
                cslot.at[slot, p], cslot.at[slot, p],
                cs_send.at[slot, d], cs_recv.at[slot, p], p,
            ).wait_recv()
        col = joined(cslot.at[slot], img_n)
        for k in range(pieces):
            cstat[slot, 0:1, k * LANES : (k + 1) * LANES] = col[k : k + 1]
        return row, col

    def spread(slot, here):
        return jnp.concatenate([row_at[slot, here, :]] * pieces, axis=1)

    row_s, col_s = gathered(1)

    def student_group(g, c):
        here = pl.ds(pl.multiple_of(g * 8, 8), 8)
        sg = s2[here, :]
        q[here, :] = jnp.exp2(sg - spread(1, here)) + jnp.exp2(sg - cstat[1, 0:1, :])
        return c

    lax.fori_loop(0, rows // 8, student_group, 0, unroll=8)
    row_t, col_t = gathered(0)

    per = rows // txt_n
    cper = cols // img_n
    wide_c = 2 * cper
    half = cper // 2
    mate = mi + 1 - 2 * mc
    high = (2 * mz) // levels
    zp = mz + high * (levels - 1 - 2 * mz)

    def real(b):
        return b + high * (levels - 1 - 2 * b)

    def rows_of(p):
        return pl.ds(pl.multiple_of(p * per, per), per)

    def cols_of(o):
        return pl.ds(pl.multiple_of(o * cper, cper), cper)

    def delta_block(b):
        first = pl.multiple_of(b * wide_c, LANES)
        group = 4 if strips % 4 == 0 else 1

        def some(g, c):
            for k in range(group):
                at = pl.ds(pl.multiple_of((g * group + k) * LANES, LANES), LANES)
                r = row_at[0, at, :]
                for n in range(wide_c // LANES):
                    cs = pl.ds(pl.multiple_of(first + n * LANES, LANES), LANES)
                    tg = t2[at, cs]
                    d = q[at, cs] - jnp.exp2(tg - r) - jnp.exp2(tg - cstat[0, 0:1, cs])
                    d = (8.0 * d).astype(jnp.bfloat16)
                    delta[at, cs] = d
                    deltat[cs, at] = d.T
            return c

        lax.fori_loop(0, strips // group, some, 0)

    x_out = []

    def text_pair(b):
        pair = pl.ds(pl.multiple_of(b * wide_c, wide_c), wide_c)
        gt[pair, :] = scale_g * jnp.dot(
            deltat[pair, :], simg[...], preferred_element_type=F32
        )
        o = 2 * b + 1 - mc
        copy = to_img(gt.at[cols_of(o), :], xr.at[b], x_send.at[b], x_recv.at[b], mate)
        copy.start()
        x_out.append(copy)

    def hop(b, h, way):
        at = pl.ds(pl.multiple_of((2 * b + mc) * cper + h * half, half), half)
        slot = zr.at[way, b, pl.ds(h * half, half), :]
        return at, slot, to_img(
            gt.at[at, :], slot, z_send.at[way, b, h], z_recv.at[way, b, h],
            mi + 4 * way - 2,
        )

    def merge_mate(b):
        to_img(xr.at[b], xr.at[b], x_send.at[b], x_recv.at[b], mate).wait_recv()
        at = cols_of(2 * b + mc)
        gt[at, :] = gt[at, :] + xr[b]

    def launch(bp):
        @pl.when(jnp.logical_and(zp == 0, bp > 0))
        def _():
            for h in range(2):
                hop(real(bp), h, 1 - high)[2].start()

    far = list(reversed(range(levels)))
    lag = 2
    for n, bp in enumerate(far):
        delta_block(real(bp))
        text_pair(real(bp))
        if n >= lag:
            merge_mate(real(far[n - lag]))
            launch(far[n - lag])

    gi_out = []
    minor = minor_of(txt_n)
    major = txt_n // minor
    my, mx = mt // minor, lax.rem(mt, minor)
    part = per // 2

    def block(y, x, w):
        return pl.ds(pl.multiple_of((y * minor + x) * per + w * part, part), part)

    ys = [lax.rem(my + d, major) for d in range(1, major)]
    xs = [lax.rem(mx + d, minor) for d in range(1, minor)]

    def image_term(y, x):
        p = y * minor + x
        gi[rows_of(p), :] = scale_g * jnp.dot(
            delta[rows_of(p), :], stxt[...], preferred_element_type=F32
        )

    def begin(copies):
        for copy in copies:
            copy.start()
        gi_out.extend(copies)

    def image_a(y, x):
        return to_txt(
            gi.at[block(y, x, 0), :], g1a.at[mx, y],
            a1_send.at[x, y], a1_recv.at[mx, y], my * minor + x,
        )

    def image_b(y, x):
        return to_txt(
            gi.at[block(y, x, 1), :], g1b.at[my, x],
            b1_send.at[y, x], b1_recv.at[my, x], y * minor + mx,
        )

    for y in ys:
        for x in xs:
            image_term(y, x)
            begin([image_a(y, x), image_b(y, x)])
    for bp in far[max(0, levels - lag) :]:
        merge_mate(real(bp))
        if bp > 1:
            launch(bp)
    for y in ys:
        image_term(y, mx)
    for x in xs:
        image_term(my, x)
    image_term(my, mx)

    def teacher_group(g, acc):
        here = pl.ds(pl.multiple_of(g * 8, 8), 8)
        tg = t2[here, :]
        gap = tg - s2[here, :]
        p_row = jnp.exp2(tg - spread(0, here))
        p_col = jnp.exp2(tg - cstat[0, 0:1, :])
        return acc + (
            p_row * (1.0 / (rows * img_n)) + p_col * (1.0 / (cols * txt_n))
        ) * gap

    total = lax.fori_loop(0, rows // 8, teacher_group, jnp.zeros((8, cols), F32), unroll=4)
    mine = (
        jnp.sum(total)
        + jnp.sum(row_s - row_t) * (1.0 / (rows * img_n * txt_n))
        + jnp.sum(col_s - col_t) * (1.0 / (cols * txt_n * img_n))
    )
    lrow[mt] = jnp.full((8, LANES), mine, F32)
    l1_out = [
        to_txt(lrow.at[mt], lrow.at[mt], l1_send.at[d], l1_recv.at[mt], p)
        for d, p in enumerate(txt_peers)
    ]
    for copy in l1_out:
        copy.start()
    for x in xs:
        begin([image_a(my, x)])
    for y in ys:
        begin([image_b(y, mx)])

    def take_a(y):
        for x in xs:
            to_txt(
                g1a.at[x, y], g1a.at[x, y], a1_send.at[x, y], a1_recv.at[x, y],
                my * minor + x,
            ).wait_recv()
            gi[block(y, mx, 0), :] = gi[block(y, mx, 0), :] + g1a[x, y]

    def take_b(x):
        for y in ys:
            to_txt(
                g1b.at[y, x], g1b.at[y, x], b1_send.at[y, x], b1_recv.at[y, x],
                y * minor + mx,
            ).wait_recv()
            gi[block(my, x, 1), :] = gi[block(my, x, 1), :] + g1b[y, x]

    def second_leg():
        for y in ys:
            take_a(y)
            begin([to_txt(
                gi.at[block(y, mx, 0), :], g2a.at[my], a2_send.at[y], a2_recv.at[my],
                y * minor + mx,
            )])
        for x in xs:
            take_b(x)
            begin([to_txt(
                gi.at[block(my, x, 1), :], g2b.at[mx], b2_send.at[x], b2_recv.at[mx],
                my * minor + x,
            )])

    def loss_leg():
        for d, p in enumerate(txt_peers):
            to_txt(lrow.at[p], lrow.at[p], l1_send.at[d], l1_recv.at[p], p).wait_recv()
        lcol[mi] = functools.reduce(jnp.add, [lrow[k] for k in range(txt_n)])
        l2_out = [
            to_img(lcol.at[mi], lcol.at[mi], l2_send.at[d], l2_recv.at[mi], p)
            for d, p in enumerate(img_peers)
        ]
        for copy in l2_out:
            copy.start()
        if levels > 1:
            launch(1)
        return l2_out

    def onward(bp, h, up):
        @pl.when(jnp.logical_and(zp < bp, zp > 0) if up else zp > bp)
        def _():
            at, slot, copy = hop(real(bp), h, 1 - high if up else high)
            copy.wait_recv()
            gt[at, :] = gt[at, :] + slot[...]
            copy.start()

    steps = [
        ((levels - 1 - bp) * 2 + h, True, bp, h) for bp in range(2, levels) for h in range(2)
    ] + [
        (bp * 2 + h + 1.5, False, bp, h) for bp in range(levels // 2) for h in range(2)
    ]
    l2_out = None
    for key, up, bp, h in sorted(steps):
        if key > 1 and l2_out is None:
            second_leg()
            l2_out = loss_leg()
        onward(bp, h, up)
    if l2_out is None:
        second_leg()
        l2_out = loss_leg()

    take_a(my)
    take_b(mx)
    for d, p in enumerate(img_peers):
        to_img(lcol.at[p], lcol.at[p], l2_send.at[d], l2_recv.at[p], p).wait_recv()
    loss_ref[...] = (0.5 * LN2) * functools.reduce(jnp.add, [lcol[k] for k in range(img_n)])

    for way in (0, 1):
        @pl.when(mz > 0 if way else mz < levels - 1)
        def _(way=way):
            for h in range(2):
                at, slot, copy = hop(mz, h, way)
                copy.wait_recv()
                gt[at, :] = gt[at, :] + slot[...]

    gtxt_ref[...] = gt[cols_of(mi), :]
    for y in ys:
        to_txt(
            g2a.at[y], g2a.at[y], a2_send.at[y], a2_recv.at[y], y * minor + mx
        ).wait_recv()
        gi[block(my, mx, 0), :] = gi[block(my, mx, 0), :] + g2a[y]
    for x in xs:
        to_txt(
            g2b.at[x], g2b.at[x], b2_send.at[x], b2_recv.at[x], my * minor + x
        ).wait_recv()
        gi[block(my, mx, 1), :] = gi[block(my, mx, 1), :] + g2b[x]
    gimg_ref[...] = gi[rows_of(mt), :]
    for b in range(levels):
        for way in (0, 1):
            @pl.when(b > mz if way else b < mz)
            def _(b=b, way=way):
                for h in range(2):
                    hop(b, h, way)[2].wait_send()

    for copy in [*stat_out, *gi_out, *x_out, *l1_out, *l2_out]:
        copy.wait_send()


def hand_over(loss, gimg, gtxt, loss_out, gimg_out, gtxt_out):
    loss_out[0, 0] = loss[0, 0]
    gimg_out[...] = gimg[...]
    gtxt_out[...] = gtxt[...]


def body(img_n, txt_n, teacher_img, teacher_txt, student_img, student_txt):
    rows, wide = teacher_img.shape
    cols, deep = student_txt.shape
    levels = img_n // 2
    vmem = pltpu.VMEM
    minor = minor_of(txt_n)
    major = txt_n // minor
    part = rows // txt_n // 2
    dma = pltpu.SemaphoreType.DMA
    bf16 = jnp.bfloat16
    loss, grad_img, grad_txt = pl.pallas_call(
        functools.partial(kernel, img_n, txt_n),
        out_shape=(
            jax.ShapeDtypeStruct((8, LANES), F32),
            jax.ShapeDtypeStruct((rows // txt_n, deep), F32),
            jax.ShapeDtypeStruct((cols // img_n, deep), F32),
        ),
        in_specs=[pl.BlockSpec(memory_space=pltpu.HBM)] * 4,
        out_specs=tuple(pl.BlockSpec(memory_space=vmem) for _ in range(3)),
        scratch_shapes=[
            vmem((rows, wide), bf16), vmem((cols, wide), bf16),
            vmem((rows, deep), bf16), vmem((cols, deep), bf16),
            vmem((rows, cols), F32), vmem((rows, cols), F32), vmem((rows, cols), F32),
            vmem((2, rows, LANES), F32), vmem((2, 8, cols), F32),
            vmem((2, txt_n, 2, rows // LANES, LANES), F32),
            vmem((2, img_n, 2, cols // LANES, LANES), F32),
            vmem((rows, cols), bf16), vmem((cols, rows), bf16),
            vmem((rows, deep), F32), vmem((minor, major, part, deep), F32),
            vmem((major, minor, part, deep), F32),
            vmem((major, part, deep), F32), vmem((minor, part, deep), F32),
            vmem((cols, deep), F32), vmem((levels, cols // img_n, deep), F32),
            vmem((2, levels, cols // img_n, deep), F32),
            vmem((txt_n, 8, LANES), F32), vmem((img_n, 8, LANES), F32),
            dma((4,)),
            dma((2, txt_n)), dma((2, txt_n)), dma((2, img_n)), dma((2, img_n)),
            dma((minor, major)), dma((minor, major)), dma((major, minor)), dma((major, minor)),
            dma((major,)), dma((major,)), dma((minor,)), dma((minor,)), dma((levels,)), dma((levels,)),
            dma((2, levels, 2)), dma((2, levels, 2)),
            dma((txt_n,)), dma((txt_n,)), dma((img_n,)), dma((img_n,)),
        ],
        compiler_params=pltpu.CompilerParams(
            collective_id=0, has_side_effects=True, vmem_limit_bytes=60 * 1024 * 1024
        ),
    )(teacher_img, teacher_txt, student_img, student_txt)
    loss, grad_img, grad_txt = pl.pallas_call(
        hand_over,
        out_shape=(
            jax.ShapeDtypeStruct((1, 1), F32),
            jax.ShapeDtypeStruct(grad_img.shape, F32),
            jax.ShapeDtypeStruct(grad_txt.shape, F32),
        ),
        in_specs=[pl.BlockSpec(memory_space=vmem)] * 3,
        out_specs=(
            pl.BlockSpec(memory_space=pltpu.SMEM),
            pl.BlockSpec(memory_space=vmem), pl.BlockSpec(memory_space=vmem),
        ),
    )(loss, grad_img, grad_txt)
    return loss.reshape(()), grad_img, grad_txt


def solution(mesh):
    placed = (P("img", None), P("txt", None), P("img", None), P("txt", None))
    return jax.shard_map(
        functools.partial(body, mesh.shape["img"], mesh.shape["txt"]),
        mesh=mesh,
        in_specs=placed,
        out_specs=(P(), P(("img", "txt"), None), P(("txt", "img"), None)),
        check_vma=False,
    )
```

```python
import functools
import math

import jax
import jax.numpy as jnp
from jax import lax
from jax.experimental import pallas as pl
from jax.experimental.pallas import tpu as pltpu
from jax.sharding import PartitionSpec as P

LANES = 128
LOG2E = math.log2(math.e)
LN2 = math.log(2.0)
MESH = pl.DeviceIdType.MESH
F32 = jnp.float32
NT = (((1,), (1,)), ((), ()))


def minor_of(n):
    return 1 << ((n.bit_length() - 1) // 2)


def kernel(
    img_n, txt_n,
    timg_hbm, ttxt_hbm, simg_hbm, stxt_hbm,
    loss_ref, gimg_ref, gtxt_ref,
    timg, ttxt, simg, stxt, t2, s2, q, row_at, row_sum, cstat, rslot, cslot, delta, deltat,
    gi, g1a, g1b, g2a, g2b, gt, xr, zr, lrow, lcol,
    in_sem, rs_send, rs_recv, cs_send, cs_recv, a1_send, a1_recv, b1_send, b1_recv,
    a2_send, a2_recv, b2_send, b2_recv, x_send, x_recv,
    z_send, z_recv, l1_send, l1_recv, l2_send, l2_recv,
):
    rows, wide = timg.shape
    cols, deep = stxt.shape
    strips = rows // LANES
    pieces = cols // LANES
    mi = lax.axis_index("img")
    mt = lax.axis_index("txt")
    levels = img_n // 2
    mz = mi // 2
    mc = lax.rem(mi, 2)
    scale_t = 3.0 / math.sqrt(wide) * LOG2E
    scale_s = 3.0 / math.sqrt(deep) * LOG2E
    scale_g = 3.0 / math.sqrt(deep)

    loads = [
        pltpu.make_async_copy(src, dst, in_sem.at[k])
        for k, (src, dst) in enumerate(
            ((simg_hbm, simg), (stxt_hbm, stxt), (timg_hbm, timg), (ttxt_hbm, ttxt))
        )
    ]
    for load in loads:
        load.start()

    barrier = pltpu.get_barrier_semaphore()
    txt_peers = [lax.rem(mt + d, txt_n) for d in range(1, txt_n)]
    img_peers = [lax.rem(mi + d, img_n) for d in range(1, img_n)]
    for p in txt_peers:
        pl.semaphore_signal(barrier, inc=1, device_id=(mi, p), device_id_type=MESH)
    for p in img_peers:
        pl.semaphore_signal(barrier, inc=1, device_id=(p, mt), device_id_type=MESH)

    def to_txt(src, dst, send, recv, p):
        return pltpu.make_async_remote_copy(
            src_ref=src, dst_ref=dst, send_sem=send, recv_sem=recv,
            device_id=(mi, p), device_id_type=MESH,
        )

    def to_img(src, dst, send, recv, p):
        return pltpu.make_async_remote_copy(
            src_ref=src, dst_ref=dst, send_sem=send, recv_sem=recv,
            device_id=(p, mt), device_id_type=MESH,
        )

    chunk = min(2 * LANES, cols)
    chunks = cols // chunk
    stat_out = []

    def tile_of(left, right, out, factor, slot, j):
        at = pl.ds(pl.multiple_of(j * chunk, chunk), chunk)
        tile = factor * lax.dot_general(
            left[...], right[at, :], NT, preferred_element_type=F32
        )
        out[:, at] = tile
        cstat[slot, 0:1, at] = jnp.max(tile, axis=0, keepdims=True)

    def lanes(x):
        return [x[:, k * LANES : (k + 1) * LANES] for k in range(pieces)]

    def group(out, slot, start, mass):
        here = pl.ds(pl.multiple_of(start, 8), 8)
        x = out[here, :]
        peak = functools.reduce(jnp.maximum, lanes(x))
        row_at[slot, here, :] = peak
        row_sum[slot, here, :] = functools.reduce(
            jnp.add, [jnp.exp2(v - peak) for v in lanes(x)]
        )
        return mass + jnp.exp2(x - cstat[slot, 0:1, :])

    def share(slot, mass):
        total = cstat[slot, 0:1, :] + jnp.log(jnp.sum(mass, axis=0, keepdims=True)) * LOG2E
        for k in range(pieces):
            cslot[slot, mi, k : k + 1, :] = total[:, k * LANES : (k + 1) * LANES]
        if slot == 1:
            pl.semaphore_wait(barrier, txt_n - 1 + img_n - 1)
        copies = [
            to_img(
                cslot.at[slot, mi], cslot.at[slot, mi],
                cs_send.at[slot, d], cs_recv.at[slot, mi], p,
            )
            for d, p in reversed(list(enumerate(img_peers)))
        ]
        for copy in copies:
            copy.start()
        stat_out.extend(copies)
        for k in range(strips):
            at = slice(k * LANES, (k + 1) * LANES)
            peaks = row_at[slot, at, :].T
            top = jnp.max(peaks, axis=0, keepdims=True)
            row = jnp.sum(row_sum[slot, at, :].T * jnp.exp2(peaks - top), axis=0, keepdims=True)
            rslot[slot, mt, k : k + 1, :] = top + jnp.log(row) * LOG2E
        copies = [
            to_txt(
                rslot.at[slot, mt], rslot.at[slot, mt],
                rs_send.at[slot, d], rs_recv.at[slot, mt], p,
            )
            for d, p in enumerate(txt_peers)
        ]
        for copy in copies:
            copy.start()
        stat_out.extend(copies)

    zero = jnp.zeros((8, cols), F32)
    loads[0].wait()
    loads[1].wait()
    lax.fori_loop(
        0, chunks, lambda j, c: (tile_of(simg, stxt, s2, scale_s, 1, j), c)[1], 0
    )
    loads[2].wait()
    loads[3].wait()

    share_rows = rows // chunks

    def both(j, mass):
        tile_of(timg, ttxt, t2, scale_t, 0, j)
        for g in range(share_rows // 8):
            mass = group(s2, 1, j * share_rows + g * 8, mass)
        return mass

    share(1, lax.fori_loop(0, chunks, both, zero))
    share(0, lax.fori_loop(
        0, rows // 8, lambda g, mass: group(t2, 0, g * 8, mass), zero, unroll=8
    ))

    def joined(slot, n):
        logs = [slot[k] for k in range(n)]
        top = functools.reduce(jnp.maximum, logs)
        mass = functools.reduce(jnp.add, [jnp.exp2(v - top) for v in logs])
        return top + jnp.log(mass) * LOG2E

    def gathered(slot):
        for d, p in enumerate(txt_peers):
            to_txt(
                rslot.at[slot, p], rslot.at[slot, p],
                rs_send.at[slot, d], rs_recv.at[slot, p], p,
            ).wait_recv()
        row = joined(rslot.at[slot], txt_n)
        for k in range(strips):
            row_at[slot, k * LANES : (k + 1) * LANES, :] = jnp.broadcast_to(
                row[k : k + 1], (LANES, LANES)
            ).T
        for d, p in enumerate(img_peers):
            to_img(
                cslot.at[slot, p], cslot.at[slot, p],
                cs_send.at[slot, d], cs_recv.at[slot, p], p,
            ).wait_recv()
        col = joined(cslot.at[slot], img_n)
        for k in range(pieces):
            cstat[slot, 0:1, k * LANES : (k + 1) * LANES] = col[k : k + 1]
        return row, col

    def spread(slot, here):
        return jnp.concatenate([row_at[slot, here, :]] * pieces, axis=1)

    row_s, col_s = gathered(1)

    def student_group(g, c):
        here = pl.ds(pl.multiple_of(g * 8, 8), 8)
        sg = s2[here, :]
        q[here, :] = jnp.exp2(sg - spread(1, here)) + jnp.exp2(sg - cstat[1, 0:1, :])
        return c

    lax.fori_loop(0, rows // 8, student_group, 0, unroll=8)
    row_t, col_t = gathered(0)

    per = rows // txt_n
    cper = cols // img_n
    wide_c = 2 * cper
    half = cper // 2
    mate = mi + 1 - 2 * mc
    high = (2 * mz) // levels
    zp = mz + high * (levels - 1 - 2 * mz)

    def real(b):
        return b + high * (levels - 1 - 2 * b)

    def rows_of(p):
        return pl.ds(pl.multiple_of(p * per, per), per)

    def cols_of(o):
        return pl.ds(pl.multiple_of(o * cper, cper), cper)

    def delta_block(b):
        first = pl.multiple_of(b * wide_c, LANES)
        group = 4 if strips % 4 == 0 else 1

        def some(g, c):
            for k in range(group):
                at = pl.ds(pl.multiple_of((g * group + k) * LANES, LANES), LANES)
                r = row_at[0, at, :]
                for n in range(wide_c // LANES):
                    cs = pl.ds(pl.multiple_of(first + n * LANES, LANES), LANES)
                    tg = t2[at, cs]
                    d = q[at, cs] - jnp.exp2(tg - r) - jnp.exp2(tg - cstat[0, 0:1, cs])
                    d = (8.0 * d).astype(jnp.bfloat16)
                    delta[at, cs] = d
                    deltat[cs, at] = d.T
            return c

        lax.fori_loop(0, strips // group, some, 0)

    x_out = []

    def text_pair(b):
        pair = pl.ds(pl.multiple_of(b * wide_c, wide_c), wide_c)
        gt[pair, :] = scale_g * jnp.dot(
            deltat[pair, :], simg[...], preferred_element_type=F32
        )
        o = 2 * b + 1 - mc
        copy = to_img(gt.at[cols_of(o), :], xr.at[b], x_send.at[b], x_recv.at[b], mate)
        copy.start()
        x_out.append(copy)

    def hop(b, h, way):
        at = pl.ds(pl.multiple_of((2 * b + mc) * cper + h * half, half), half)
        slot = zr.at[way, b, pl.ds(h * half, half), :]
        return at, slot, to_img(
            gt.at[at, :], slot, z_send.at[way, b, h], z_recv.at[way, b, h],
            mi + 4 * way - 2,
        )

    def merge_mate(b):
        to_img(xr.at[b], xr.at[b], x_send.at[b], x_recv.at[b], mate).wait_recv()
        at = cols_of(2 * b + mc)
        gt[at, :] = gt[at, :] + xr[b]

    def launch(bp):
        @pl.when(jnp.logical_and(zp == 0, bp > 0))
        def _():
            for h in range(2):
                hop(real(bp), h, 1 - high)[2].start()

    far = list(reversed(range(levels)))
    lag = 2
    for n, bp in enumerate(far):
        delta_block(real(bp))
        text_pair(real(bp))
        if n >= lag:
            merge_mate(real(far[n - lag]))
            launch(far[n - lag])

    gi_out = []
    minor = minor_of(txt_n)
    major = txt_n // minor
    my, mx = mt // minor, lax.rem(mt, minor)
    part = per // 2

    def block(y, x, w):
        return pl.ds(pl.multiple_of((y * minor + x) * per + w * part, part), part)

    ys = [lax.rem(my + d, major) for d in range(1, major)]
    xs = [lax.rem(mx + d, minor) for d in range(1, minor)]

    def image_term(y, x):
        p = y * minor + x
        gi[rows_of(p), :] = scale_g * jnp.dot(
            delta[rows_of(p), :], stxt[...], preferred_element_type=F32
        )

    def begin(copies):
        for copy in copies:
            copy.start()
        gi_out.extend(copies)

    def image_a(y, x):
        return to_txt(
            gi.at[block(y, x, 0), :], g1a.at[mx, y],
            a1_send.at[x, y], a1_recv.at[mx, y], my * minor + x,
        )

    def image_b(y, x):
        return to_txt(
            gi.at[block(y, x, 1), :], g1b.at[my, x],
            b1_send.at[y, x], b1_recv.at[my, x], y * minor + mx,
        )

    for y in ys:
        for x in xs:
            image_term(y, x)
            begin([image_a(y, x), image_b(y, x)])
    for bp in far[max(0, levels - lag) :]:
        merge_mate(real(bp))
        if bp > 1:
            launch(bp)
    for y in ys:
        image_term(y, mx)
    for x in xs:
        image_term(my, x)
    image_term(my, mx)

    def teacher_group(g, acc):
        here = pl.ds(pl.multiple_of(g * 8, 8), 8)
        tg = t2[here, :]
        gap = tg - s2[here, :]
        p_row = jnp.exp2(tg - spread(0, here))
        p_col = jnp.exp2(tg - cstat[0, 0:1, :])
        return acc + (
            p_row * (1.0 / (rows * img_n)) + p_col * (1.0 / (cols * txt_n))
        ) * gap

    total = lax.fori_loop(0, rows // 8, teacher_group, jnp.zeros((8, cols), F32), unroll=4)
    mine = (
        jnp.sum(total)
        + jnp.sum(row_s - row_t) * (1.0 / (rows * img_n * txt_n))
        + jnp.sum(col_s - col_t) * (1.0 / (cols * txt_n * img_n))
    )
    lrow[mt] = jnp.full((8, LANES), mine, F32)
    l1_out = [
        to_txt(lrow.at[mt], lrow.at[mt], l1_send.at[d], l1_recv.at[mt], p)
        for d, p in enumerate(txt_peers)
    ]
    for copy in l1_out:
        copy.start()
    for x in xs:
        begin([image_a(my, x)])
    for y in ys:
        begin([image_b(y, mx)])

    def take_a(y):
        for x in xs:
            to_txt(
                g1a.at[x, y], g1a.at[x, y], a1_send.at[x, y], a1_recv.at[x, y],
                my * minor + x,
            ).wait_recv()
            gi[block(y, mx, 0), :] = gi[block(y, mx, 0), :] + g1a[x, y]

    def take_b(x):
        for y in ys:
            to_txt(
                g1b.at[y, x], g1b.at[y, x], b1_send.at[y, x], b1_recv.at[y, x],
                y * minor + mx,
            ).wait_recv()
            gi[block(my, x, 1), :] = gi[block(my, x, 1), :] + g1b[y, x]

    def second_leg():
        for y in ys:
            take_a(y)
            begin([to_txt(
                gi.at[block(y, mx, 0), :], g2a.at[my], a2_send.at[y], a2_recv.at[my],
                y * minor + mx,
            )])
        for x in xs:
            take_b(x)
            begin([to_txt(
                gi.at[block(my, x, 1), :], g2b.at[mx], b2_send.at[x], b2_recv.at[mx],
                my * minor + x,
            )])

    def loss_leg():
        for d, p in enumerate(txt_peers):
            to_txt(lrow.at[p], lrow.at[p], l1_send.at[d], l1_recv.at[p], p).wait_recv()
        lcol[mi] = functools.reduce(jnp.add, [lrow[k] for k in range(txt_n)])
        l2_out = [
            to_img(lcol.at[mi], lcol.at[mi], l2_send.at[d], l2_recv.at[mi], p)
            for d, p in enumerate(img_peers)
        ]
        for copy in l2_out:
            copy.start()
        if levels > 1:
            launch(1)
        return l2_out

    def onward(bp, h, up):
        @pl.when(jnp.logical_and(zp < bp, zp > 0) if up else zp > bp)
        def _():
            at, slot, copy = hop(real(bp), h, 1 - high if up else high)
            copy.wait_recv()
            gt[at, :] = gt[at, :] + slot[...]
            copy.start()

    steps = [
        ((levels - 1 - bp) * 2 + h, True, bp, h) for bp in range(2, levels) for h in range(2)
    ] + [
        (bp * 2 + h + 1.5, False, bp, h) for bp in range(levels // 2) for h in range(2)
    ]
    l2_out = None
    for key, up, bp, h in sorted(steps):
        if key > 1 and l2_out is None:
            second_leg()
            l2_out = loss_leg()
        onward(bp, h, up)
    if l2_out is None:
        second_leg()
        l2_out = loss_leg()

    take_a(my)
    take_b(mx)
    for d, p in enumerate(img_peers):
        to_img(lcol.at[p], lcol.at[p], l2_send.at[d], l2_recv.at[p], p).wait_recv()
    loss_ref[...] = (0.5 * LN2) * functools.reduce(jnp.add, [lcol[k] for k in range(img_n)])

    for way in (0, 1):
        @pl.when(mz > 0 if way else mz < levels - 1)
        def _(way=way):
            for h in range(2):
                at, slot, copy = hop(mz, h, way)
                copy.wait_recv()
                gt[at, :] = gt[at, :] + slot[...]

    gtxt_ref[...] = gt[cols_of(mi), :]
    for y in ys:
        to_txt(
            g2a.at[y], g2a.at[y], a2_send.at[y], a2_recv.at[y], y * minor + mx
        ).wait_recv()
        gi[block(my, mx, 0), :] = gi[block(my, mx, 0), :] + g2a[y]
    for x in xs:
        to_txt(
            g2b.at[x], g2b.at[x], b2_send.at[x], b2_recv.at[x], my * minor + x
        ).wait_recv()
        gi[block(my, mx, 1), :] = gi[block(my, mx, 1), :] + g2b[x]
    gimg_ref[...] = gi[rows_of(mt), :]
    for b in range(levels):
        for way in (0, 1):
            @pl.when(b > mz if way else b < mz)
            def _(b=b, way=way):
                for h in range(2):
                    hop(b, h, way)[2].wait_send()

    for copy in [*stat_out, *gi_out, *x_out, *l1_out, *l2_out]:
        copy.wait_send()


def hand_over(loss, gimg, gtxt, loss_out, gimg_out, gtxt_out):
    loss_out[0, 0] = loss[0, 0]
    gimg_out[...] = gimg[...]
    gtxt_out[...] = gtxt[...]


def body(img_n, txt_n, teacher_img, teacher_txt, student_img, student_txt):
    rows, wide = teacher_img.shape
    cols, deep = student_txt.shape
    levels = img_n // 2
    vmem = pltpu.VMEM
    minor = minor_of(txt_n)
    major = txt_n // minor
    part = rows // txt_n // 2
    dma = pltpu.SemaphoreType.DMA
    bf16 = jnp.bfloat16
    loss, grad_img, grad_txt = pl.pallas_call(
        functools.partial(kernel, img_n, txt_n),
        out_shape=(
            jax.ShapeDtypeStruct((8, LANES), F32),
            jax.ShapeDtypeStruct((rows // txt_n, deep), F32),
            jax.ShapeDtypeStruct((cols // img_n, deep), F32),
        ),
        in_specs=[pl.BlockSpec(memory_space=pltpu.HBM)] * 4,
        out_specs=tuple(pl.BlockSpec(memory_space=vmem) for _ in range(3)),
        scratch_shapes=[
            vmem((rows, wide), bf16), vmem((cols, wide), bf16),
            vmem((rows, deep), bf16), vmem((cols, deep), bf16),
            vmem((rows, cols), F32), vmem((rows, cols), F32), vmem((rows, cols), F32),
            vmem((2, rows, LANES), F32), vmem((2, rows, LANES), F32), vmem((2, 8, cols), F32),
            vmem((2, txt_n, rows // LANES, LANES), F32),
            vmem((2, img_n, cols // LANES, LANES), F32),
            vmem((rows, cols), bf16), vmem((cols, rows), bf16),
            vmem((rows, deep), F32), vmem((minor, major, part, deep), F32),
            vmem((major, minor, part, deep), F32),
            vmem((major, part, deep), F32), vmem((minor, part, deep), F32),
            vmem((cols, deep), F32), vmem((levels, cols // img_n, deep), F32),
            vmem((2, levels, cols // img_n, deep), F32),
            vmem((txt_n, 8, LANES), F32), vmem((img_n, 8, LANES), F32),
            dma((4,)),
            dma((2, txt_n)), dma((2, txt_n)), dma((2, img_n)), dma((2, img_n)),
            dma((minor, major)), dma((minor, major)), dma((major, minor)), dma((major, minor)),
            dma((major,)), dma((major,)), dma((minor,)), dma((minor,)), dma((levels,)), dma((levels,)),
            dma((2, levels, 2)), dma((2, levels, 2)),
            dma((txt_n,)), dma((txt_n,)), dma((img_n,)), dma((img_n,)),
        ],
        compiler_params=pltpu.CompilerParams(
            collective_id=0, has_side_effects=True, vmem_limit_bytes=60 * 1024 * 1024
        ),
    )(teacher_img, teacher_txt, student_img, student_txt)
    loss, grad_img, grad_txt = pl.pallas_call(
        hand_over,
        out_shape=(
            jax.ShapeDtypeStruct((1, 1), F32),
            jax.ShapeDtypeStruct(grad_img.shape, F32),
            jax.ShapeDtypeStruct(grad_txt.shape, F32),
        ),
        in_specs=[pl.BlockSpec(memory_space=vmem)] * 3,
        out_specs=(
            pl.BlockSpec(memory_space=pltpu.SMEM),
            pl.BlockSpec(memory_space=vmem), pl.BlockSpec(memory_space=vmem),
        ),
    )(loss, grad_img, grad_txt)
    return loss.reshape(()), grad_img, grad_txt


def solution(mesh):
    placed = (P("img", None), P("txt", None), P("img", None), P("txt", None))
    return jax.shard_map(
        functools.partial(body, mesh.shape["img"], mesh.shape["txt"]),
        mesh=mesh,
        in_specs=placed,
        out_specs=(P(), P(("img", "txt"), None), P(("txt", "img"), None)),
        check_vma=False,
    )
```

```python
import functools
import math

import jax
import jax.numpy as jnp
from jax import lax
from jax.experimental import pallas as pl
from jax.experimental.pallas import tpu as pltpu
from jax.sharding import PartitionSpec as P

LANES = 128
LOG2E = math.log2(math.e)
LN2 = math.log(2.0)
MESH = pl.DeviceIdType.MESH
F32 = jnp.float32
NT = (((1,), (1,)), ((), ()))


def minor_of(n):
    return 1 << ((n.bit_length() - 1) // 2)


def kernel(
    img_n, txt_n,
    timg_hbm, ttxt_hbm, simg_hbm, stxt_hbm,
    loss_ref, gimg_ref, gtxt_ref,
    timg, ttxt, simg, stxt, t2, s2, q, row_at, row_sum, cstat, rslot, cslot, delta, deltat,
    gi, g1a, g1b, g2a, g2b, gt, xr, zr, lrow, lcol,
    in_sem, rs_send, rs_recv, cs_send, cs_recv, a1_send, a1_recv, b1_send, b1_recv,
    a2_send, a2_recv, b2_send, b2_recv, x_send, x_recv,
    z_send, z_recv, l1_send, l1_recv, l2_send, l2_recv,
):
    rows, wide = timg.shape
    cols, deep = stxt.shape
    strips = rows // LANES
    pieces = cols // LANES
    mi = lax.axis_index("img")
    mt = lax.axis_index("txt")
    levels = img_n // 2
    mz = mi // 2
    mc = lax.rem(mi, 2)
    scale_t = 3.0 / math.sqrt(wide) * LOG2E
    scale_s = 3.0 / math.sqrt(deep) * LOG2E
    scale_g = 3.0 / math.sqrt(deep)

    loads = [
        pltpu.make_async_copy(src, dst, in_sem.at[k])
        for k, (src, dst) in enumerate(
            ((simg_hbm, simg), (stxt_hbm, stxt), (timg_hbm, timg), (ttxt_hbm, ttxt))
        )
    ]
    for load in loads:
        load.start()

    barrier = pltpu.get_barrier_semaphore()
    txt_peers = [lax.rem(mt + d, txt_n) for d in range(1, txt_n)]
    img_peers = [lax.rem(mi + d, img_n) for d in range(1, img_n)]
    for p in txt_peers:
        pl.semaphore_signal(barrier, inc=1, device_id=(mi, p), device_id_type=MESH)
    for p in img_peers:
        pl.semaphore_signal(barrier, inc=1, device_id=(p, mt), device_id_type=MESH)

    def to_txt(src, dst, send, recv, p):
        return pltpu.make_async_remote_copy(
            src_ref=src, dst_ref=dst, send_sem=send, recv_sem=recv,
            device_id=(mi, p), device_id_type=MESH,
        )

    def to_img(src, dst, send, recv, p):
        return pltpu.make_async_remote_copy(
            src_ref=src, dst_ref=dst, send_sem=send, recv_sem=recv,
            device_id=(p, mt), device_id_type=MESH,
        )

    chunk = min(2 * LANES, cols)
    chunks = cols // chunk
    stat_out = []

    def tile_of(left, right, out, factor, slot, at):
        tile = factor * lax.dot_general(
            left[...], right[at, :], NT, preferred_element_type=F32
        )
        out[:, at] = tile
        cstat[slot, 0:1, at] = jnp.max(tile, axis=0, keepdims=True)

    def lanes(x):
        return [x[:, k * LANES : (k + 1) * LANES] for k in range(pieces)]

    def row_group(out, slot, start):
        here = pl.ds(pl.multiple_of(start, 8), 8)
        x = out[here, :]
        peak = functools.reduce(jnp.maximum, lanes(x))
        row_at[slot, here, :] = peak
        row_sum[slot, here, :] = functools.reduce(
            jnp.add, [jnp.exp2(v - peak) for v in lanes(x)]
        )
        return x

    def col_log(slot, at, mass):
        total = cstat[slot, 0:1, at] + jnp.log(jnp.sum(mass, axis=0, keepdims=True)) * LOG2E
        for k in range(at.start // LANES, at.stop // LANES):
            here = slice(k * LANES - at.start, (k + 1) * LANES - at.start)
            cslot[slot, mi, k : k + 1, :] = total[:, here]

    def send_cols(slot):
        copies = [
            to_img(
                cslot.at[slot, mi], cslot.at[slot, mi],
                cs_send.at[slot, d], cs_recv.at[slot, mi], p,
            )
            for d, p in reversed(list(enumerate(img_peers)))
        ]
        for copy in copies:
            copy.start()
        stat_out.extend(copies)

    def send_rows(slot):
        for k in range(strips):
            at = slice(k * LANES, (k + 1) * LANES)
            peaks = row_at[slot, at, :].T
            top = jnp.max(peaks, axis=0, keepdims=True)
            row = jnp.sum(row_sum[slot, at, :].T * jnp.exp2(peaks - top), axis=0, keepdims=True)
            rslot[slot, mt, k : k + 1, :] = top + jnp.log(row) * LOG2E
        copies = [
            to_txt(
                rslot.at[slot, mt], rslot.at[slot, mt],
                rs_send.at[slot, d], rs_recv.at[slot, mt], p,
            )
            for d, p in enumerate(txt_peers)
        ]
        for copy in copies:
            copy.start()
        stat_out.extend(copies)

    tiles = [slice(j * chunk, (j + 1) * chunk) for j in range(chunks)]
    loads[0].wait()
    loads[1].wait()
    lax.fori_loop(0, chunks, lambda j, c: (tile_of(
        simg, stxt, s2, scale_s, 1, pl.ds(pl.multiple_of(j * chunk, chunk), chunk)
    ), c)[1], 0)
    loads[2].wait()
    loads[3].wait()

    def col_mass(at):
        mass = jnp.zeros((8, chunk), F32)
        for g in range(rows // 8):
            mass = mass + jnp.exp2(t2[g * 8 : g * 8 + 8, at] - cstat[0, 0:1, at])
        col_log(0, at, mass)

    early = max(1, chunks // 2)
    share_rows = rows // early
    mass = jnp.zeros((8, cols), F32)
    for j, at in enumerate(tiles):
        if j == early:
            col_log(1, slice(0, cols), mass)
            pl.semaphore_wait(barrier, txt_n - 1 + img_n - 1)
            send_cols(1)
            send_rows(1)
        if j > 0:
            col_mass(tiles[j - 1])
        tile_of(timg, ttxt, t2, scale_t, 0, at)
        if j < early:
            for g in range(share_rows // 8):
                x = row_group(s2, 1, j * share_rows + g * 8)
                mass = mass + jnp.exp2(x - cstat[1, 0:1, :])
    col_mass(tiles[-1])
    send_cols(0)
    lax.fori_loop(0, rows // 8, lambda g, c: (row_group(t2, 0, g * 8), c)[1], 0, unroll=8)
    send_rows(0)

    def joined(slot, n):
        logs = [slot[k] for k in range(n)]
        top = functools.reduce(jnp.maximum, logs)
        mass = functools.reduce(jnp.add, [jnp.exp2(v - top) for v in logs])
        return top + jnp.log(mass) * LOG2E

    def gathered(slot):
        for d, p in enumerate(txt_peers):
            to_txt(
                rslot.at[slot, p], rslot.at[slot, p],
                rs_send.at[slot, d], rs_recv.at[slot, p], p,
            ).wait_recv()
        row = joined(rslot.at[slot], txt_n)
        for k in range(strips):
            row_at[slot, k * LANES : (k + 1) * LANES, :] = jnp.broadcast_to(
                row[k : k + 1], (LANES, LANES)
            ).T
        for d, p in enumerate(img_peers):
            to_img(
                cslot.at[slot, p], cslot.at[slot, p],
                cs_send.at[slot, d], cs_recv.at[slot, p], p,
            ).wait_recv()
        col = joined(cslot.at[slot], img_n)
        for k in range(pieces):
            cstat[slot, 0:1, k * LANES : (k + 1) * LANES] = col[k : k + 1]
        return row, col

    def spread(slot, here):
        return jnp.concatenate([row_at[slot, here, :]] * pieces, axis=1)

    row_s, col_s = gathered(1)

    def student_group(g, c):
        here = pl.ds(pl.multiple_of(g * 8, 8), 8)
        sg = s2[here, :]
        q[here, :] = jnp.exp2(sg - spread(1, here)) + jnp.exp2(sg - cstat[1, 0:1, :])
        return c

    lax.fori_loop(0, rows // 8, student_group, 0, unroll=4)
    row_t, col_t = gathered(0)

    per = rows // txt_n
    cper = cols // img_n
    wide_c = 2 * cper
    half = cper // 2
    mate = mi + 1 - 2 * mc
    high = (2 * mz) // levels
    zp = mz + high * (levels - 1 - 2 * mz)

    def real(b):
        return b + high * (levels - 1 - 2 * b)

    def rows_of(p):
        return pl.ds(pl.multiple_of(p * per, per), per)

    def cols_of(o):
        return pl.ds(pl.multiple_of(o * cper, cper), cper)

    def delta_tiles(row_starts, b):
        for r0 in row_starts:
            at = pl.ds(pl.multiple_of(r0, LANES), LANES)
            r = row_at[0, at, :]
            for n in range(wide_c // LANES):
                cs = pl.ds(pl.multiple_of(b * wide_c + n * LANES, LANES), LANES)
                tg = t2[at, cs]
                d = q[at, cs] - jnp.exp2(tg - r) - jnp.exp2(tg - cstat[0, 0:1, cs])
                d = (8.0 * d).astype(jnp.bfloat16)
                delta[at, cs] = d
                deltat[cs, at] = d.T

    def delta_block(b):
        group = 4 if strips % 4 == 0 else 1
        lax.fori_loop(
            0, strips // group,
            lambda g, c: (
                delta_tiles([(g * group + k) * LANES for k in range(group)], b), c
            )[1], 0,
        )

    x_out = []

    def text_pair(b):
        pair = pl.ds(pl.multiple_of(b * wide_c, wide_c), wide_c)
        gt[pair, :] = scale_g * jnp.dot(
            deltat[pair, :], simg[...], preferred_element_type=F32
        )
        o = 2 * b + 1 - mc
        copy = to_img(gt.at[cols_of(o), :], xr.at[b], x_send.at[b], x_recv.at[b], mate)
        copy.start()
        x_out.append(copy)

    def hop(b, h, way):
        at = pl.ds(pl.multiple_of((2 * b + mc) * cper + h * half, half), half)
        slot = zr.at[way, b, pl.ds(h * half, half), :]
        return at, slot, to_img(
            gt.at[at, :], slot, z_send.at[way, b, h], z_recv.at[way, b, h],
            mi + 4 * way - 2,
        )

    def merge_mate(b):
        to_img(xr.at[b], xr.at[b], x_send.at[b], x_recv.at[b], mate).wait_recv()
        at = cols_of(2 * b + mc)
        gt[at, :] = gt[at, :] + xr[b]

    def launch(bp):
        @pl.when(jnp.logical_and(zp == 0, bp > 0))
        def _():
            for h in range(2):
                hop(real(bp), h, 1 - high)[2].start()

    gi_out = []
    minor = minor_of(txt_n)
    major = txt_n // minor
    my, mx = mt // minor, lax.rem(mt, minor)
    part = per // 2

    def block(y, x, w):
        return pl.ds(pl.multiple_of((y * minor + x) * per + w * part, part), part)

    ys = [lax.rem(my + d, major) for d in range(1, major)]
    xs = [lax.rem(mx + d, minor) for d in range(1, minor)]

    def image_term(y, x):
        p = y * minor + x
        gi[rows_of(p), :] = scale_g * jnp.dot(
            delta[rows_of(p), :], stxt[...], preferred_element_type=F32
        )

    def begin(copies):
        for copy in copies:
            copy.start()
        gi_out.extend(copies)

    def image_a(y, x):
        return to_txt(
            gi.at[block(y, x, 0), :], g1a.at[mx, y],
            a1_send.at[x, y], a1_recv.at[mx, y], my * minor + x,
        )

    def image_b(y, x):
        return to_txt(
            gi.at[block(y, x, 1), :], g1b.at[my, x],
            b1_send.at[y, x], b1_recv.at[my, x], y * minor + mx,
        )

    far = list(reversed(range(levels)))
    diag = [(y, x) for y in ys for x in xs]
    side = [(y, mx) for y in ys] + [(my, x) for x in xs] + [(my, mx)]
    lag = min(2, levels)
    fine = per % LANES == 0

    def strips_of(blocks):
        return [
            (y * minor + x) * per + k * LANES for y, x in blocks for k in range(per // LANES)
        ]

    def images():
        for y, x in diag:
            image_term(y, x)
            begin([image_a(y, x), image_b(y, x)])

    for bp in far[:lag]:
        delta_block(real(bp))
        text_pair(real(bp))
    if fine:
        for bp in far[lag:]:
            delta_tiles(strips_of(diag), real(bp))
        images()
    for n, bp in enumerate(far[lag:]):
        merge_mate(real(far[n]))
        launch(far[n])
        if fine:
            delta_tiles(strips_of(side), real(bp))
        else:
            delta_block(real(bp))
        text_pair(real(bp))
    if not fine:
        images()
    for bp in far[max(0, levels - lag) :]:
        merge_mate(real(bp))
        if bp > 1:
            launch(bp)
    for y, x in side:
        image_term(y, x)

    def teacher_group(g, acc):
        here = pl.ds(pl.multiple_of(g * 8, 8), 8)
        tg = t2[here, :]
        gap = tg - s2[here, :]
        p_row = jnp.exp2(tg - spread(0, here))
        p_col = jnp.exp2(tg - cstat[0, 0:1, :])
        return acc + (
            p_row * (1.0 / (rows * img_n)) + p_col * (1.0 / (cols * txt_n))
        ) * gap

    total = lax.fori_loop(0, rows // 8, teacher_group, jnp.zeros((8, cols), F32), unroll=4)
    mine = (
        jnp.sum(total)
        + jnp.sum(row_s - row_t) * (1.0 / (rows * img_n * txt_n))
        + jnp.sum(col_s - col_t) * (1.0 / (cols * txt_n * img_n))
    )
    lrow[mt] = jnp.full((8, LANES), mine, F32)
    l1_out = [
        to_txt(lrow.at[mt], lrow.at[mt], l1_send.at[d], l1_recv.at[mt], p)
        for d, p in enumerate(txt_peers)
    ]
    for copy in l1_out:
        copy.start()
    for x in xs:
        begin([image_a(my, x)])
    for y in ys:
        begin([image_b(y, mx)])

    def take_a(y):
        for x in xs:
            to_txt(
                g1a.at[x, y], g1a.at[x, y], a1_send.at[x, y], a1_recv.at[x, y],
                my * minor + x,
            ).wait_recv()
            gi[block(y, mx, 0), :] = gi[block(y, mx, 0), :] + g1a[x, y]

    def take_b(x):
        for y in ys:
            to_txt(
                g1b.at[y, x], g1b.at[y, x], b1_send.at[y, x], b1_recv.at[y, x],
                y * minor + mx,
            ).wait_recv()
            gi[block(my, x, 1), :] = gi[block(my, x, 1), :] + g1b[y, x]

    def second_leg():
        for y in ys:
            take_a(y)
            begin([to_txt(
                gi.at[block(y, mx, 0), :], g2a.at[my], a2_send.at[y], a2_recv.at[my],
                y * minor + mx,
            )])
        for x in xs:
            take_b(x)
            begin([to_txt(
                gi.at[block(my, x, 1), :], g2b.at[mx], b2_send.at[x], b2_recv.at[mx],
                my * minor + x,
            )])

    def loss_leg():
        for d, p in enumerate(txt_peers):
            to_txt(lrow.at[p], lrow.at[p], l1_send.at[d], l1_recv.at[p], p).wait_recv()
        lcol[mi] = functools.reduce(jnp.add, [lrow[k] for k in range(txt_n)])
        l2_out = [
            to_img(lcol.at[mi], lcol.at[mi], l2_send.at[d], l2_recv.at[mi], p)
            for d, p in enumerate(img_peers)
        ]
        for copy in l2_out:
            copy.start()
        if levels > 1:
            launch(1)
        return l2_out

    def onward(bp, h, up):
        @pl.when(jnp.logical_and(zp < bp, zp > 0) if up else zp > bp)
        def _():
            at, slot, copy = hop(real(bp), h, 1 - high if up else high)
            copy.wait_recv()
            gt[at, :] = gt[at, :] + slot[...]
            copy.start()

    steps = [
        ((levels - 1 - bp) * 2 + h, True, bp, h) for bp in range(2, levels) for h in range(2)
    ] + [
        (bp * 2 + h + 1.5, False, bp, h) for bp in range(levels // 2) for h in range(2)
    ]
    l2_out = None
    for key, up, bp, h in sorted(steps):
        if key > 1 and l2_out is None:
            second_leg()
            l2_out = loss_leg()
        onward(bp, h, up)
    if l2_out is None:
        second_leg()
        l2_out = loss_leg()

    take_a(my)
    take_b(mx)
    for d, p in enumerate(img_peers):
        to_img(lcol.at[p], lcol.at[p], l2_send.at[d], l2_recv.at[p], p).wait_recv()
    loss_ref[...] = (0.5 * LN2) * functools.reduce(jnp.add, [lcol[k] for k in range(img_n)])

    for way in (0, 1):
        @pl.when(mz > 0 if way else mz < levels - 1)
        def _(way=way):
            for h in range(2):
                at, slot, copy = hop(mz, h, way)
                copy.wait_recv()
                gt[at, :] = gt[at, :] + slot[...]

    gtxt_ref[...] = gt[cols_of(mi), :]
    for y in ys:
        to_txt(
            g2a.at[y], g2a.at[y], a2_send.at[y], a2_recv.at[y], y * minor + mx
        ).wait_recv()
        gi[block(my, mx, 0), :] = gi[block(my, mx, 0), :] + g2a[y]
    for x in xs:
        to_txt(
            g2b.at[x], g2b.at[x], b2_send.at[x], b2_recv.at[x], my * minor + x
        ).wait_recv()
        gi[block(my, mx, 1), :] = gi[block(my, mx, 1), :] + g2b[x]
    gimg_ref[...] = gi[rows_of(mt), :]
    for b in range(levels):
        for way in (0, 1):
            @pl.when(b > mz if way else b < mz)
            def _(b=b, way=way):
                for h in range(2):
                    hop(b, h, way)[2].wait_send()

    for copy in [*stat_out, *gi_out, *x_out, *l1_out, *l2_out]:
        copy.wait_send()


def hand_over(loss, gimg, gtxt, loss_out, gimg_out, gtxt_out, sem):
    copies = [
        pltpu.make_async_copy(gimg, gimg_out, sem.at[0]),
        pltpu.make_async_copy(gtxt, gtxt_out, sem.at[1]),
    ]
    for copy in copies:
        copy.start()
    loss_out[0, 0] = loss[0, 0]
    for copy in copies:
        copy.wait()


def body(img_n, txt_n, teacher_img, teacher_txt, student_img, student_txt):
    rows, wide = teacher_img.shape
    cols, deep = student_txt.shape
    levels = img_n // 2
    vmem = pltpu.VMEM
    minor = minor_of(txt_n)
    major = txt_n // minor
    part = rows // txt_n // 2
    dma = pltpu.SemaphoreType.DMA
    bf16 = jnp.bfloat16
    loss, grad_img, grad_txt = pl.pallas_call(
        functools.partial(kernel, img_n, txt_n),
        out_shape=(
            jax.ShapeDtypeStruct((8, LANES), F32),
            jax.ShapeDtypeStruct((rows // txt_n, deep), F32),
            jax.ShapeDtypeStruct((cols // img_n, deep), F32),
        ),
        in_specs=[pl.BlockSpec(memory_space=pltpu.HBM)] * 4,
        out_specs=tuple(pl.BlockSpec(memory_space=vmem) for _ in range(3)),
        scratch_shapes=[
            vmem((rows, wide), bf16), vmem((cols, wide), bf16),
            vmem((rows, deep), bf16), vmem((cols, deep), bf16),
            vmem((rows, cols), F32), vmem((rows, cols), F32), vmem((rows, cols), F32),
            vmem((2, rows, LANES), F32), vmem((2, rows, LANES), F32), vmem((2, 8, cols), F32),
            vmem((2, txt_n, rows // LANES, LANES), F32),
            vmem((2, img_n, cols // LANES, LANES), F32),
            vmem((rows, cols), bf16), vmem((cols, rows), bf16),
            vmem((rows, deep), F32), vmem((minor, major, part, deep), F32),
            vmem((major, minor, part, deep), F32),
            vmem((major, part, deep), F32), vmem((minor, part, deep), F32),
            vmem((cols, deep), F32), vmem((levels, cols // img_n, deep), F32),
            vmem((2, levels, cols // img_n, deep), F32),
            vmem((txt_n, 8, LANES), F32), vmem((img_n, 8, LANES), F32),
            dma((4,)),
            dma((2, txt_n)), dma((2, txt_n)), dma((2, img_n)), dma((2, img_n)),
            dma((minor, major)), dma((minor, major)), dma((major, minor)), dma((major, minor)),
            dma((major,)), dma((major,)), dma((minor,)), dma((minor,)), dma((levels,)), dma((levels,)),
            dma((2, levels, 2)), dma((2, levels, 2)),
            dma((txt_n,)), dma((txt_n,)), dma((img_n,)), dma((img_n,)),
        ],
        compiler_params=pltpu.CompilerParams(
            collective_id=0, has_side_effects=True, vmem_limit_bytes=48 * 1024 * 1024
        ),
    )(*[pltpu.with_memory_space_constraint(v, pltpu.HBM) for v in (teacher_img, teacher_txt, student_img, student_txt)])
    loss, grad_img, grad_txt = pl.pallas_call(
        hand_over,
        out_shape=(
            jax.ShapeDtypeStruct((1, 1), F32),
            jax.ShapeDtypeStruct(grad_img.shape, F32),
            jax.ShapeDtypeStruct(grad_txt.shape, F32),
        ),
        in_specs=[pl.BlockSpec(memory_space=vmem)] * 3,
        out_specs=(
            pl.BlockSpec(memory_space=pltpu.SMEM),
            pl.BlockSpec(memory_space=pltpu.HBM), pl.BlockSpec(memory_space=pltpu.HBM),
        ),
        scratch_shapes=[dma((2,))],
        compiler_params=pltpu.CompilerParams(vmem_limit_bytes=1024 * 1024),
    )(loss, grad_img, grad_txt)
    return loss.reshape(()), grad_img, grad_txt


def solution(mesh):
    placed = (P("img", None), P("txt", None), P("img", None), P("txt", None))
    return jax.shard_map(
        functools.partial(body, mesh.shape["img"], mesh.shape["txt"]),
        mesh=mesh,
        in_specs=placed,
        out_specs=(P(), P(("img", "txt"), None), P(("txt", "img"), None)),
        check_vma=False,
    )
```

```python
import functools
import math

import jax
import jax.numpy as jnp
from jax import lax
from jax.experimental import pallas as pl
from jax.experimental.pallas import tpu as pltpu
from jax.sharding import PartitionSpec as P

LANES = 128
LOG2E = math.log2(math.e)
LN2 = math.log(2.0)
MESH = pl.DeviceIdType.MESH
F32 = jnp.float32
NT = (((1,), (1,)), ((), ()))


def minor_of(n):
    return 1 << ((n.bit_length() - 1) // 2)


def kernel(
    img_n, txt_n,
    timg_hbm, ttxt_hbm, simg_hbm, stxt_hbm,
    loss_ref, gimg_ref, gtxt_ref,
    timg, ttxt, simg, stxt, t2, s2, q, row_at, row_sum, cstat, rslot, cslot, delta, deltat,
    gi, g1a, g1b, g2a, g2b, gt, xr, zr, lrow, lcol,
    in_sem, rs_send, rs_recv, cs_send, cs_recv, a1_send, a1_recv, b1_send, b1_recv,
    a2_send, a2_recv, b2_send, b2_recv, x_send, x_recv,
    z_send, z_recv, l1_send, l1_recv, l2_send, l2_recv,
):
    rows, wide = timg.shape
    cols, deep = stxt.shape
    strips = rows // LANES
    pieces = cols // LANES
    mi = lax.axis_index("img")
    mt = lax.axis_index("txt")
    levels = img_n // 2
    mz = mi // 2
    mc = lax.rem(mi, 2)
    scale_t = 3.0 / math.sqrt(wide) * LOG2E
    scale_s = 3.0 / math.sqrt(deep) * LOG2E
    scale_g = 3.0 / math.sqrt(deep)

    loads = [
        pltpu.make_async_copy(src, dst, in_sem.at[k])
        for k, (src, dst) in enumerate(
            ((simg_hbm, simg), (stxt_hbm, stxt), (timg_hbm, timg), (ttxt_hbm, ttxt))
        )
    ]
    for load in loads:
        load.start()

    barrier = pltpu.get_barrier_semaphore()
    txt_peers = [lax.rem(mt + d, txt_n) for d in range(1, txt_n)]
    img_peers = [lax.rem(mi + d, img_n) for d in range(1, img_n)]
    for p in txt_peers:
        pl.semaphore_signal(barrier, inc=1, device_id=(mi, p), device_id_type=MESH)
    for p in img_peers:
        pl.semaphore_signal(barrier, inc=1, device_id=(p, mt), device_id_type=MESH)

    def to_txt(src, dst, send, recv, p):
        return pltpu.make_async_remote_copy(
            src_ref=src, dst_ref=dst, send_sem=send, recv_sem=recv,
            device_id=(mi, p), device_id_type=MESH,
        )

    def to_img(src, dst, send, recv, p):
        return pltpu.make_async_remote_copy(
            src_ref=src, dst_ref=dst, send_sem=send, recv_sem=recv,
            device_id=(p, mt), device_id_type=MESH,
        )

    chunk = min(2 * LANES, cols)
    chunks = cols // chunk
    stat_out = []

    def tile_of(left, right, out, factor, slot, at):
        tile = factor * lax.dot_general(
            left[...], right[at, :], NT, preferred_element_type=F32
        )
        out[:, at] = tile
        cstat[slot, 0:1, at] = jnp.max(tile, axis=0, keepdims=True)

    def lanes(x):
        return [x[:, k * LANES : (k + 1) * LANES] for k in range(pieces)]

    def row_group(out, slot, start):
        here = pl.ds(pl.multiple_of(start, 8), 8)
        x = out[here, :]
        peak = functools.reduce(jnp.maximum, lanes(x))
        row_at[slot, here, :] = peak
        row_sum[slot, here, :] = functools.reduce(
            jnp.add, [jnp.exp2(v - peak) for v in lanes(x)]
        )
        return x

    def col_log(slot, at, mass):
        total = cstat[slot, 0:1, at] + jnp.log(jnp.sum(mass, axis=0, keepdims=True)) * LOG2E
        for k in range(at.start // LANES, at.stop // LANES):
            here = slice(k * LANES - at.start, (k + 1) * LANES - at.start)
            cslot[slot, mi, k : k + 1, :] = total[:, here]

    def send_cols(slot):
        copies = [
            to_img(
                cslot.at[slot, mi], cslot.at[slot, mi],
                cs_send.at[slot, d], cs_recv.at[slot, mi], p,
            )
            for d, p in reversed(list(enumerate(img_peers)))
        ]
        for copy in copies:
            copy.start()
        stat_out.extend(copies)

    def send_rows(slot):
        for k in range(strips):
            at = slice(k * LANES, (k + 1) * LANES)
            peaks = row_at[slot, at, :].T
            top = jnp.max(peaks, axis=0, keepdims=True)
            row = jnp.sum(row_sum[slot, at, :].T * jnp.exp2(peaks - top), axis=0, keepdims=True)
            rslot[slot, mt, k : k + 1, :] = top + jnp.log(row) * LOG2E
        copies = [
            to_txt(
                rslot.at[slot, mt], rslot.at[slot, mt],
                rs_send.at[slot, d], rs_recv.at[slot, mt], p,
            )
            for d, p in enumerate(txt_peers)
        ]
        for copy in copies:
            copy.start()
        stat_out.extend(copies)

    tiles = [slice(j * chunk, (j + 1) * chunk) for j in range(chunks)]
    loads[0].wait()
    loads[1].wait()
    lax.fori_loop(0, chunks, lambda j, c: (tile_of(
        simg, stxt, s2, scale_s, 1, pl.ds(pl.multiple_of(j * chunk, chunk), chunk)
    ), c)[1], 0)
    loads[2].wait()
    loads[3].wait()

    def col_mass(at):
        mass = jnp.zeros((8, chunk), F32)
        for g in range(rows // 8):
            mass = mass + jnp.exp2(t2[g * 8 : g * 8 + 8, at] - cstat[0, 0:1, at])
        col_log(0, at, mass)

    early = max(1, chunks // 2)
    share_rows = rows // early
    mass = jnp.zeros((8, cols), F32)
    for j, at in enumerate(tiles):
        if j == early:
            col_log(1, slice(0, cols), mass)
            pl.semaphore_wait(barrier, txt_n - 1 + img_n - 1)
            send_cols(1)
            send_rows(1)
        if j > 0:
            col_mass(tiles[j - 1])
        tile_of(timg, ttxt, t2, scale_t, 0, at)
        if j < early:
            for g in range(share_rows // 8):
                x = row_group(s2, 1, j * share_rows + g * 8)
                mass = mass + jnp.exp2(x - cstat[1, 0:1, :])
    col_mass(tiles[-1])
    send_cols(0)
    lax.fori_loop(0, rows // 8, lambda g, c: (row_group(t2, 0, g * 8), c)[1], 0, unroll=8)
    send_rows(0)

    def joined(slot, n):
        logs = [slot[k] for k in range(n)]
        top = functools.reduce(jnp.maximum, logs)
        mass = functools.reduce(jnp.add, [jnp.exp2(v - top) for v in logs])
        return top + jnp.log(mass) * LOG2E

    def gathered(slot):
        for d, p in enumerate(txt_peers):
            to_txt(
                rslot.at[slot, p], rslot.at[slot, p],
                rs_send.at[slot, d], rs_recv.at[slot, p], p,
            ).wait_recv()
        row = joined(rslot.at[slot], txt_n)
        for k in range(strips):
            row_at[slot, k * LANES : (k + 1) * LANES, :] = jnp.broadcast_to(
                row[k : k + 1], (LANES, LANES)
            ).T
        for d, p in enumerate(img_peers):
            to_img(
                cslot.at[slot, p], cslot.at[slot, p],
                cs_send.at[slot, d], cs_recv.at[slot, p], p,
            ).wait_recv()
        col = joined(cslot.at[slot], img_n)
        for k in range(pieces):
            cstat[slot, 0:1, k * LANES : (k + 1) * LANES] = col[k : k + 1]
        return row, col

    def spread(slot, here):
        return jnp.concatenate([row_at[slot, here, :]] * pieces, axis=1)

    row_s, col_s = gathered(1)

    def student_group(g, c):
        here = pl.ds(pl.multiple_of(g * 8, 8), 8)
        sg = s2[here, :]
        q[here, :] = jnp.exp2(sg - spread(1, here)) + jnp.exp2(sg - cstat[1, 0:1, :])
        return c

    lax.fori_loop(0, rows // 8, student_group, 0, unroll=4)
    row_t, col_t = gathered(0)

    per = rows // txt_n
    cper = cols // img_n
    wide_c = 2 * cper
    half = cper // 2
    mate = mi + 1 - 2 * mc
    high = (2 * mz) // levels
    zp = mz + high * (levels - 1 - 2 * mz)

    def real(b):
        return b + high * (levels - 1 - 2 * b)

    def rows_of(p):
        return pl.ds(pl.multiple_of(p * per, per), per)

    def cols_of(o):
        return pl.ds(pl.multiple_of(o * cper, cper), cper)

    def delta_tile(r0, b, n, keep):
        at = pl.ds(pl.multiple_of(r0, LANES), LANES)
        for k in range(wide_c // LANES):
            cs = pl.ds(pl.multiple_of(b * wide_c + k * LANES, LANES), LANES)
            tg = t2[at, cs]
            d = q[at, cs] - jnp.exp2(tg - row_at[0, at, :]) - jnp.exp2(tg - cstat[0, 0:1, cs])
            d = (8.0 * d).astype(jnp.bfloat16)
            keep(cs, d)
            deltat[n, k * LANES : (k + 1) * LANES, at] = d.T

    def delta_blocks(found, b, n):
        for slot, (y, x) in found:
            for k in range(per // LANES):
                def keep(cs, d, slot=slot, k=k):
                    delta[slot, k * LANES : (k + 1) * LANES, cs] = d

                delta_tile((y * minor + x) * per + k * LANES, b, n, keep)

    def delta_strips(b, n):
        def one(g, c):
            def keep(cs, d):
                for k in range(LANES // per):
                    delta[g * (LANES // per) + k, :, cs] = d[k * per : (k + 1) * per]

            delta_tile(g * LANES, b, n, keep)
            return c

        lax.fori_loop(0, strips, one, 0)

    x_out = []

    def text_pair(b, n):
        pair = pl.ds(pl.multiple_of(b * wide_c, wide_c), wide_c)
        gt[pair, :] = scale_g * jnp.dot(
            deltat[n], simg[...], preferred_element_type=F32
        )

    def text_mate(b):
        o = 2 * b + 1 - mc
        copy = to_img(gt.at[cols_of(o), :], xr.at[b], x_send.at[b], x_recv.at[b], mate)
        copy.start()
        x_out.append(copy)

    def hop(b, h, way):
        at = pl.ds(pl.multiple_of((2 * b + mc) * cper + h * half, half), half)
        slot = zr.at[way, b, pl.ds(h * half, half), :]
        return at, slot, to_img(
            gt.at[at, :], slot, z_send.at[way, b, h], z_recv.at[way, b, h],
            mi + 4 * way - 2,
        )

    def merge_mate(b):
        to_img(xr.at[b], xr.at[b], x_send.at[b], x_recv.at[b], mate).wait_recv()
        at = cols_of(2 * b + mc)
        gt[at, :] = gt[at, :] + xr[b]

    def launch(bp):
        @pl.when(jnp.logical_and(zp == 0, bp > 0))
        def _():
            for h in range(2):
                hop(real(bp), h, 1 - high)[2].start()

    gi_out = []
    minor = minor_of(txt_n)
    major = txt_n // minor
    my, mx = mt // minor, lax.rem(mt, minor)
    part = per // 2

    def block(y, x, w):
        return pl.ds(pl.multiple_of((y * minor + x) * per + w * part, part), part)

    ys = [lax.rem(my + d, major) for d in range(1, major)]
    xs = [lax.rem(mx + d, minor) for d in range(1, minor)]

    def image_term(y, x, slot):
        gi[rows_of(y * minor + x), :] = scale_g * jnp.dot(
            delta[slot], stxt[...], preferred_element_type=F32
        )

    def begin(copies):
        for copy in copies:
            copy.start()
        gi_out.extend(copies)

    def image_a(y, x):
        return to_txt(
            gi.at[block(y, x, 0), :], g1a.at[mx, y],
            a1_send.at[x, y], a1_recv.at[mx, y], my * minor + x,
        )

    def image_b(y, x):
        return to_txt(
            gi.at[block(y, x, 1), :], g1b.at[my, x],
            b1_send.at[y, x], b1_recv.at[my, x], y * minor + mx,
        )

    far = list(reversed(range(levels)))
    diag = [(y, x) for y in ys for x in xs]
    side = [(y, mx) for y in ys] + [(my, x) for x in xs] + [(my, mx)]
    blocks = list(enumerate(diag + side))
    fine = per % LANES == 0

    def images(found):
        for slot, (y, x) in found:
            image_term(y, x, slot if fine else y * minor + x)

    def first_images():
        for y, x in diag:
            begin([image_a(y, x), image_b(y, x)])

    def pass_on(bp):
        merge_mate(real(bp))
        if bp > 1:
            launch(bp)

    if fine:
        corner, rest = blocks[: len(diag)], blocks[len(diag) :]
        delta_blocks(blocks, real(far[0]), 0)
        text_pair(real(far[0]), 0)
        text_mate(real(far[0]))
        for n, bp in enumerate(far[1:]):
            delta_blocks(corner, real(bp), n + 1)
        if levels > 1:
            delta_blocks(rest, real(far[1]), 1)
        images(corner)
        first_images()
        if levels > 2:
            pass_on(far[0])
        for n in range(1, levels):
            if n + 1 < levels:
                delta_blocks(rest, real(far[n + 1]), n + 1)
            text_pair(real(far[n]), n)
            text_mate(real(far[n]))
            if n > 2:
                pass_on(far[n - 2])
        images(rest[:1])
        for bp in far[max(0, levels - 2) :]:
            pass_on(bp)
        images(rest[1:])
    else:
        for n, bp in enumerate(far):
            delta_strips(real(bp), n)
            text_pair(real(bp), n)
            text_mate(real(bp))
            if n > 1:
                pass_on(far[n - 2])
        images(blocks[: len(diag)])
        first_images()
        for bp in far[max(0, levels - 2) :]:
            pass_on(bp)
        images(blocks[len(diag) :])

    def teacher_group(g, acc):
        here = pl.ds(pl.multiple_of(g * 8, 8), 8)
        tg = t2[here, :]
        gap = tg - s2[here, :]
        p_row = jnp.exp2(tg - spread(0, here))
        p_col = jnp.exp2(tg - cstat[0, 0:1, :])
        return acc + (
            p_row * (1.0 / (rows * img_n)) + p_col * (1.0 / (cols * txt_n))
        ) * gap

    total = lax.fori_loop(0, rows // 8, teacher_group, jnp.zeros((8, cols), F32), unroll=8)
    mine = (
        jnp.sum(total)
        + jnp.sum(row_s - row_t) * (1.0 / (rows * img_n * txt_n))
        + jnp.sum(col_s - col_t) * (1.0 / (cols * txt_n * img_n))
    )
    lrow[mt] = jnp.full((8, LANES), mine, F32)
    l1_out = [
        to_txt(lrow.at[mt], lrow.at[mt], l1_send.at[d], l1_recv.at[mt], p)
        for d, p in enumerate(txt_peers)
    ]
    for copy in l1_out:
        copy.start()
    for x in xs:
        begin([image_a(my, x)])
    for y in ys:
        begin([image_b(y, mx)])

    def take_a(y):
        for x in xs:
            to_txt(
                g1a.at[x, y], g1a.at[x, y], a1_send.at[x, y], a1_recv.at[x, y],
                my * minor + x,
            ).wait_recv()
            gi[block(y, mx, 0), :] = gi[block(y, mx, 0), :] + g1a[x, y]

    def take_b(x):
        for y in ys:
            to_txt(
                g1b.at[y, x], g1b.at[y, x], b1_send.at[y, x], b1_recv.at[y, x],
                y * minor + mx,
            ).wait_recv()
            gi[block(my, x, 1), :] = gi[block(my, x, 1), :] + g1b[y, x]

    def second_leg():
        for y in ys:
            take_a(y)
            begin([to_txt(
                gi.at[block(y, mx, 0), :], g2a.at[my], a2_send.at[y], a2_recv.at[my],
                y * minor + mx,
            )])
        for x in xs:
            take_b(x)
            begin([to_txt(
                gi.at[block(my, x, 1), :], g2b.at[mx], b2_send.at[x], b2_recv.at[mx],
                my * minor + x,
            )])

    def loss_leg():
        for d, p in enumerate(txt_peers):
            to_txt(lrow.at[p], lrow.at[p], l1_send.at[d], l1_recv.at[p], p).wait_recv()
        lcol[mi] = functools.reduce(jnp.add, [lrow[k] for k in range(txt_n)])
        l2_out = [
            to_img(lcol.at[mi], lcol.at[mi], l2_send.at[d], l2_recv.at[mi], p)
            for d, p in enumerate(img_peers)
        ]
        for copy in l2_out:
            copy.start()
        if levels > 1:
            launch(1)
        return l2_out

    def onward(bp, h, up):
        @pl.when(jnp.logical_and(zp < bp, zp > 0) if up else zp > bp)
        def _():
            at, slot, copy = hop(real(bp), h, 1 - high if up else high)
            copy.wait_recv()
            gt[at, :] = gt[at, :] + slot[...]
            copy.start()

    steps = [
        ((levels - 1 - bp) * 2 + h, True, bp, h) for bp in range(2, levels) for h in range(2)
    ] + [
        (bp * 2 + h + 1.5, False, bp, h) for bp in range(levels // 2) for h in range(2)
    ]
    l2_out = None
    for key, up, bp, h in sorted(steps):
        if key > 1 and l2_out is None:
            second_leg()
            l2_out = loss_leg()
        onward(bp, h, up)
    if l2_out is None:
        second_leg()
        l2_out = loss_leg()

    take_a(my)
    take_b(mx)
    for d, p in enumerate(img_peers):
        to_img(lcol.at[p], lcol.at[p], l2_send.at[d], l2_recv.at[p], p).wait_recv()
    loss_ref[...] = (0.5 * LN2) * functools.reduce(jnp.add, [lcol[k] for k in range(img_n)])

    for way in (0, 1):
        @pl.when(mz > 0 if way else mz < levels - 1)
        def _(way=way):
            for h in range(2):
                at, slot, copy = hop(mz, h, way)
                copy.wait_recv()
                gt[at, :] = gt[at, :] + slot[...]

    gtxt_ref[...] = gt[cols_of(mi), :]
    for y in ys:
        to_txt(
            g2a.at[y], g2a.at[y], a2_send.at[y], a2_recv.at[y], y * minor + mx
        ).wait_recv()
        gi[block(my, mx, 0), :] = gi[block(my, mx, 0), :] + g2a[y]
    for x in xs:
        to_txt(
            g2b.at[x], g2b.at[x], b2_send.at[x], b2_recv.at[x], my * minor + x
        ).wait_recv()
        gi[block(my, mx, 1), :] = gi[block(my, mx, 1), :] + g2b[x]
    gimg_ref[...] = gi[rows_of(mt), :]
    for b in range(levels):
        for way in (0, 1):
            @pl.when(b > mz if way else b < mz)
            def _(b=b, way=way):
                for h in range(2):
                    hop(b, h, way)[2].wait_send()

    for copy in [*stat_out, *gi_out, *x_out, *l1_out, *l2_out]:
        copy.wait_send()


def hand_over(loss, gimg, gtxt, loss_out, gimg_out, gtxt_out, sem):
    copies = [
        pltpu.make_async_copy(gimg, gimg_out, sem.at[0]),
        pltpu.make_async_copy(gtxt, gtxt_out, sem.at[1]),
    ]
    for copy in copies:
        copy.start()
    loss_out[0, 0] = loss[0, 0]
    for copy in copies:
        copy.wait()


def body(img_n, txt_n, teacher_img, teacher_txt, student_img, student_txt):
    rows, wide = teacher_img.shape
    cols, deep = student_txt.shape
    levels = img_n // 2
    vmem = pltpu.VMEM
    minor = minor_of(txt_n)
    major = txt_n // minor
    part = rows // txt_n // 2
    dma = pltpu.SemaphoreType.DMA
    bf16 = jnp.bfloat16
    loss, grad_img, grad_txt = pl.pallas_call(
        functools.partial(kernel, img_n, txt_n),
        out_shape=(
            jax.ShapeDtypeStruct((8, LANES), F32),
            jax.ShapeDtypeStruct((rows // txt_n, deep), F32),
            jax.ShapeDtypeStruct((cols // img_n, deep), F32),
        ),
        in_specs=[pl.BlockSpec(memory_space=pltpu.HBM)] * 4,
        out_specs=tuple(pl.BlockSpec(memory_space=vmem) for _ in range(3)),
        scratch_shapes=[
            vmem((rows, wide), bf16), vmem((cols, wide), bf16),
            vmem((rows, deep), bf16), vmem((cols, deep), bf16),
            vmem((rows, cols), F32), vmem((rows, cols), F32), vmem((rows, cols), F32),
            vmem((2, rows, LANES), F32), vmem((2, rows, LANES), F32), vmem((2, 8, cols), F32),
            vmem((2, txt_n, rows // LANES, LANES), F32),
            vmem((2, img_n, cols // LANES, LANES), F32),
            vmem((txt_n, rows // txt_n, cols), bf16), vmem((levels, cols // levels, rows), bf16),
            vmem((rows, deep), F32), vmem((minor, major, part, deep), F32),
            vmem((major, minor, part, deep), F32),
            vmem((major, part, deep), F32), vmem((minor, part, deep), F32),
            vmem((cols, deep), F32), vmem((levels, cols // img_n, deep), F32),
            vmem((2, levels, cols // img_n, deep), F32),
            vmem((txt_n, 8, LANES), F32), vmem((img_n, 8, LANES), F32),
            dma((4,)),
            dma((2, txt_n)), dma((2, txt_n)), dma((2, img_n)), dma((2, img_n)),
            dma((minor, major)), dma((minor, major)), dma((major, minor)), dma((major, minor)),
            dma((major,)), dma((major,)), dma((minor,)), dma((minor,)), dma((levels,)), dma((levels,)),
            dma((2, levels, 2)), dma((2, levels, 2)),
            dma((txt_n,)), dma((txt_n,)), dma((img_n,)), dma((img_n,)),
        ],
        compiler_params=pltpu.CompilerParams(
            collective_id=0, has_side_effects=True, vmem_limit_bytes=48 * 1024 * 1024
        ),
    )(*[pltpu.with_memory_space_constraint(v, pltpu.HBM) for v in (teacher_img, teacher_txt, student_img, student_txt)])
    loss, grad_img, grad_txt = pl.pallas_call(
        hand_over,
        out_shape=(
            jax.ShapeDtypeStruct((1, 1), F32),
            jax.ShapeDtypeStruct(grad_img.shape, F32),
            jax.ShapeDtypeStruct(grad_txt.shape, F32),
        ),
        in_specs=[pl.BlockSpec(memory_space=vmem)] * 3,
        out_specs=(
            pl.BlockSpec(memory_space=pltpu.SMEM),
            pl.BlockSpec(memory_space=pltpu.HBM), pl.BlockSpec(memory_space=pltpu.HBM),
        ),
        scratch_shapes=[dma((2,))],
        compiler_params=pltpu.CompilerParams(vmem_limit_bytes=1024 * 1024),
    )(loss, grad_img, grad_txt)
    return loss.reshape(()), grad_img, grad_txt


def solution(mesh):
    placed = (P("img", None), P("txt", None), P("img", None), P("txt", None))
    return jax.shard_map(
        functools.partial(body, mesh.shape["img"], mesh.shape["txt"]),
        mesh=mesh,
        in_specs=placed,
        out_specs=(P(), P(("img", "txt"), None), P(("txt", "img"), None)),
        check_vma=False,
    )
```

```python
import functools
import math

import jax
import jax.numpy as jnp
from jax import lax
from jax.experimental import pallas as pl
from jax.experimental.pallas import tpu as pltpu
from jax.sharding import PartitionSpec as P

LANES = 128
LOG2E = math.log2(math.e)
LN2 = math.log(2.0)
MESH = pl.DeviceIdType.MESH
F32 = jnp.float32
NT = (((1,), (1,)), ((), ()))


def minor_of(n):
    return 1 << ((n.bit_length() - 1) // 2)


def kernel(
    img_n, txt_n,
    timg_hbm, ttxt_hbm, simg_hbm, stxt_hbm,
    loss_ref, gimg_ref, gtxt_ref,
    timg, ttxt, simg, stxt, t2, s2, q, row_at, row_sum, cstat, rslot, cslot, delta, deltat,
    gi, g1a, g1b, g2a, g2b, gt, xr, zr, lrow, lcol,
    in_sem, rs_send, rs_recv, cs_send, cs_recv, a1_send, a1_recv, b1_send, b1_recv,
    a2_send, a2_recv, b2_send, b2_recv, x_send, x_recv,
    z_send, z_recv, l1_send, l1_recv, l2_send, l2_recv,
):
    rows, wide = timg.shape
    cols, deep = stxt.shape
    strips = rows // LANES
    pieces = cols // LANES
    mi = lax.axis_index("img")
    mt = lax.axis_index("txt")
    levels = img_n // 2
    mz = mi // 2
    mc = lax.rem(mi, 2)
    scale_t = 3.0 / math.sqrt(wide) * LOG2E
    scale_s = 3.0 / math.sqrt(deep) * LOG2E
    scale_g = 3.0 / math.sqrt(deep)

    loads = [
        pltpu.make_async_copy(src, dst, in_sem.at[k])
        for k, (src, dst) in enumerate(
            ((simg_hbm, simg), (stxt_hbm, stxt), (timg_hbm, timg), (ttxt_hbm, ttxt))
        )
    ]
    for load in loads:
        load.start()

    barrier = pltpu.get_barrier_semaphore()
    txt_peers = [lax.rem(mt + d, txt_n) for d in range(1, txt_n)]
    step = 1 + (1 - (2 * mz) // levels) * (img_n - 2)
    img_peers = [lax.rem(mi + d * step, img_n) for d in range(1, img_n)]
    for p in txt_peers:
        pl.semaphore_signal(barrier, inc=1, device_id=(mi, p), device_id_type=MESH)
    for p in img_peers:
        pl.semaphore_signal(barrier, inc=1, device_id=(p, mt), device_id_type=MESH)

    def to_txt(src, dst, send, recv, p):
        return pltpu.make_async_remote_copy(
            src_ref=src, dst_ref=dst, send_sem=send, recv_sem=recv,
            device_id=(mi, p), device_id_type=MESH,
        )

    def to_img(src, dst, send, recv, p):
        return pltpu.make_async_remote_copy(
            src_ref=src, dst_ref=dst, send_sem=send, recv_sem=recv,
            device_id=(p, mt), device_id_type=MESH,
        )

    chunk = min(2 * LANES, cols)
    chunks = cols // chunk
    stat_out = []

    def tile_of(left, right, out, factor, slot, at):
        tile = factor * lax.dot_general(
            left[...], right[at, :], NT, preferred_element_type=F32
        )
        out[:, at] = tile
        cstat[slot, 0:1, at] = jnp.max(tile, axis=0, keepdims=True)

    def lanes(x):
        return [x[:, k * LANES : (k + 1) * LANES] for k in range(pieces)]

    def row_group(out, slot, start):
        here = pl.ds(pl.multiple_of(start, 8), 8)
        x = out[here, :]
        peak = functools.reduce(jnp.maximum, lanes(x))
        row_at[slot, here, :] = peak
        row_sum[slot, here, :] = functools.reduce(
            jnp.add, [jnp.exp2(v - peak) for v in lanes(x)]
        )
        return x

    def col_log(slot, at, mass):
        total = cstat[slot, 0:1, at] + jnp.log(jnp.sum(mass, axis=0, keepdims=True)) * LOG2E
        for k in range(at.start // LANES, at.stop // LANES):
            here = slice(k * LANES - at.start, (k + 1) * LANES - at.start)
            cslot[slot, mi, k : k + 1, :] = total[:, here]

    def send_cols(slot):
        copies = [
            to_img(
                cslot.at[slot, mi], cslot.at[slot, mi],
                cs_send.at[slot, d], cs_recv.at[slot, mi], p,
            )
            for d, p in enumerate(img_peers)
        ]
        for copy in copies:
            copy.start()
        stat_out.extend(copies)

    def send_rows(slot):
        for k in range(strips):
            at = slice(k * LANES, (k + 1) * LANES)
            peaks = row_at[slot, at, :].T
            top = jnp.max(peaks, axis=0, keepdims=True)
            row = jnp.sum(row_sum[slot, at, :].T * jnp.exp2(peaks - top), axis=0, keepdims=True)
            rslot[slot, mt, k : k + 1, :] = top + jnp.log(row) * LOG2E
        copies = [
            to_txt(
                rslot.at[slot, mt], rslot.at[slot, mt],
                rs_send.at[slot, d], rs_recv.at[slot, mt], p,
            )
            for d, p in enumerate(txt_peers)
        ]
        for copy in copies:
            copy.start()
        stat_out.extend(copies)

    tiles = [slice(j * chunk, (j + 1) * chunk) for j in range(chunks)]
    loads[0].wait()
    loads[1].wait()
    for at in tiles:
        tile_of(simg, stxt, s2, scale_s, 1, at)
    loads[2].wait()
    loads[3].wait()

    def col_mass(at):
        mass = jnp.zeros((8, chunk), F32)
        for g in range(rows // 8):
            mass = mass + jnp.exp2(t2[g * 8 : g * 8 + 8, at] - cstat[0, 0:1, at])
        col_log(0, at, mass)

    early = max(1, chunks // 2)
    share_rows = rows // early
    mass = jnp.zeros((8, cols), F32)
    for j, at in enumerate(tiles):
        if j == early:
            col_log(1, slice(0, cols), mass)
            pl.semaphore_wait(barrier, txt_n - 1 + img_n - 1)
            send_cols(1)
            send_rows(1)
        if j > 0:
            col_mass(tiles[j - 1])
        tile_of(timg, ttxt, t2, scale_t, 0, at)
        if j < early:
            for g in range(share_rows // 8):
                x = row_group(s2, 1, j * share_rows + g * 8)
                mass = mass + jnp.exp2(x - cstat[1, 0:1, :])
    col_mass(tiles[-1])
    send_cols(0)
    lax.fori_loop(0, rows // 8, lambda g, c: (row_group(t2, 0, g * 8), c)[1], 0, unroll=8)
    send_rows(0)

    def joined(slot, n):
        logs = [slot[k] for k in range(n)]
        top = functools.reduce(jnp.maximum, logs)
        mass = functools.reduce(jnp.add, [jnp.exp2(v - top) for v in logs])
        return top + jnp.log(mass) * LOG2E

    def gathered(slot):
        for d, p in enumerate(txt_peers):
            to_txt(
                rslot.at[slot, p], rslot.at[slot, p],
                rs_send.at[slot, d], rs_recv.at[slot, p], p,
            ).wait_recv()
        row = joined(rslot.at[slot], txt_n)
        for k in range(strips):
            row_at[slot, k * LANES : (k + 1) * LANES, :] = jnp.broadcast_to(
                row[k : k + 1], (LANES, LANES)
            ).T
        for d, p in enumerate(img_peers):
            to_img(
                cslot.at[slot, p], cslot.at[slot, p],
                cs_send.at[slot, d], cs_recv.at[slot, p], p,
            ).wait_recv()
        col = joined(cslot.at[slot], img_n)
        for k in range(pieces):
            cstat[slot, 0:1, k * LANES : (k + 1) * LANES] = col[k : k + 1]
        return row, col

    def spread(slot, here):
        return jnp.concatenate([row_at[slot, here, :]] * pieces, axis=1)

    row_s, col_s = gathered(1)

    def student_group(g, c):
        here = pl.ds(pl.multiple_of(g * 8, 8), 8)
        sg = s2[here, :]
        q[here, :] = jnp.exp2(sg - spread(1, here)) + jnp.exp2(sg - cstat[1, 0:1, :])
        return c

    lax.fori_loop(0, rows // 8, student_group, 0, unroll=4)
    row_t, col_t = gathered(0)

    per = rows // txt_n
    cper = cols // img_n
    wide_c = 2 * cper
    half = cper // 2
    mate = mi + 1 - 2 * mc
    high = (2 * mz) // levels
    zp = mz + high * (levels - 1 - 2 * mz)

    def real(b):
        return b + high * (levels - 1 - 2 * b)

    def rows_of(p):
        return pl.ds(pl.multiple_of(p * per, per), per)

    def cols_of(o):
        return pl.ds(pl.multiple_of(o * cper, cper), cper)

    def delta_tile(r0, b, n, keep):
        at = pl.ds(pl.multiple_of(r0, LANES), LANES)
        for k in range(wide_c // LANES):
            cs = pl.ds(pl.multiple_of(b * wide_c + k * LANES, LANES), LANES)
            tg = t2[at, cs]
            d = q[at, cs] - jnp.exp2(tg - row_at[0, at, :]) - jnp.exp2(tg - cstat[0, 0:1, cs])
            d = (8.0 * d).astype(jnp.bfloat16)
            keep(cs, d)
            deltat[n, k * LANES : (k + 1) * LANES, at] = d.T

    def delta_blocks(found, b, n):
        for slot, (y, x) in found:
            for k in range(per // LANES):
                def keep(cs, d, slot=slot, k=k):
                    delta[slot, k * LANES : (k + 1) * LANES, cs] = d

                delta_tile((y * minor + x) * per + k * LANES, b, n, keep)

    def delta_strips(b, n):
        def one(g, c):
            def keep(cs, d):
                for k in range(LANES // per):
                    delta[g * (LANES // per) + k, :, cs] = d[k * per : (k + 1) * per]

            delta_tile(g * LANES, b, n, keep)
            return c

        lax.fori_loop(0, strips, one, 0)

    x_out = []

    def text_pair(b, n):
        pair = pl.ds(pl.multiple_of(b * wide_c, wide_c), wide_c)
        gt[pair, :] = scale_g * jnp.dot(
            deltat[n], simg[...], preferred_element_type=F32
        )

    def text_mate(b):
        o = 2 * b + 1 - mc
        copy = to_img(gt.at[cols_of(o), :], xr.at[b], x_send.at[b], x_recv.at[b], mate)
        copy.start()
        x_out.append(copy)

    def hop(b, h, way):
        at = pl.ds(pl.multiple_of((2 * b + mc) * cper + h * half, half), half)
        slot = zr.at[way, b, pl.ds(h * half, half), :]
        return at, slot, to_img(
            gt.at[at, :], slot, z_send.at[way, b, h], z_recv.at[way, b, h],
            mi + 4 * way - 2,
        )

    def merge_mate(b):
        to_img(xr.at[b], xr.at[b], x_send.at[b], x_recv.at[b], mate).wait_recv()
        at = cols_of(2 * b + mc)
        gt[at, :] = gt[at, :] + xr[b]

    def launch(bp):
        @pl.when(jnp.logical_and(zp == 0, bp > 0))
        def _():
            for h in range(2):
                hop(real(bp), h, 1 - high)[2].start()

    gi_out = []
    minor = minor_of(txt_n)
    major = txt_n // minor
    my, mx = mt // minor, lax.rem(mt, minor)
    part = per // 2

    def block(y, x, w):
        return pl.ds(pl.multiple_of((y * minor + x) * per + w * part, part), part)

    ys = [lax.rem(my + d, major) for d in range(1, major)]
    xs = [lax.rem(mx + d, minor) for d in range(1, minor)]

    def image_term(y, x, slot):
        gi[rows_of(y * minor + x), :] = scale_g * jnp.dot(
            delta[slot], stxt[...], preferred_element_type=F32
        )

    def begin(copies):
        for copy in copies:
            copy.start()
        gi_out.extend(copies)

    def image_a(y, x):
        return to_txt(
            gi.at[block(y, x, 0), :], g1a.at[mx, y],
            a1_send.at[x, y], a1_recv.at[mx, y], my * minor + x,
        )

    def image_b(y, x):
        return to_txt(
            gi.at[block(y, x, 1), :], g1b.at[my, x],
            b1_send.at[y, x], b1_recv.at[my, x], y * minor + mx,
        )

    far = list(reversed(range(levels)))
    diag = [(y, x) for y in ys for x in xs]
    side = [(y, mx) for y in ys] + [(my, x) for x in xs] + [(my, mx)]
    blocks = list(enumerate(diag + side))
    fine = per % LANES == 0

    def images(found):
        for slot, (y, x) in found:
            image_term(y, x, slot if fine else y * minor + x)

    def first_images():
        for y, x in diag:
            begin([image_a(y, x), image_b(y, x)])

    def pass_on(bp):
        merge_mate(real(bp))
        if bp > 1:
            launch(bp)

    if fine:
        corner, rest = blocks[: len(diag)], blocks[len(diag) :]
        delta_blocks(blocks, real(far[0]), 0)
        text_pair(real(far[0]), 0)
        text_mate(real(far[0]))
        for n, bp in enumerate(far[1:]):
            delta_blocks(corner, real(bp), n + 1)
        if levels > 1:
            delta_blocks(rest, real(far[1]), 1)
        images(corner)
        first_images()
        if levels > 2:
            pass_on(far[0])
        for n in range(1, levels):
            if n + 1 < levels:
                delta_blocks(rest, real(far[n + 1]), n + 1)
            text_pair(real(far[n]), n)
            text_mate(real(far[n]))
            if n > 2:
                pass_on(far[n - 2])
        images(rest[:1])
        for bp in far[max(0, levels - 2) :]:
            pass_on(bp)
        images(rest[1:])
    else:
        for n, bp in enumerate(far):
            delta_strips(real(bp), n)
            text_pair(real(bp), n)
            text_mate(real(bp))
            if n > 1:
                pass_on(far[n - 2])
        images(blocks[: len(diag)])
        first_images()
        for bp in far[max(0, levels - 2) :]:
            pass_on(bp)
        images(blocks[len(diag) :])

    def teacher_group(g, acc):
        here = pl.ds(pl.multiple_of(g * 8, 8), 8)
        tg = t2[here, :]
        gap = tg - s2[here, :]
        p_row = jnp.exp2(tg - spread(0, here))
        p_col = jnp.exp2(tg - cstat[0, 0:1, :])
        return acc + (
            p_row * (1.0 / (rows * img_n)) + p_col * (1.0 / (cols * txt_n))
        ) * gap

    total = lax.fori_loop(0, rows // 8, teacher_group, jnp.zeros((8, cols), F32), unroll=8)
    mine = (
        jnp.sum(total)
        + jnp.sum(row_s - row_t) * (1.0 / (rows * img_n * txt_n))
        + jnp.sum(col_s - col_t) * (1.0 / (cols * txt_n * img_n))
    )
    lrow[mt] = jnp.full((8, LANES), mine, F32)
    l1_out = [
        to_txt(lrow.at[mt], lrow.at[mt], l1_send.at[d], l1_recv.at[mt], p)
        for d, p in enumerate(txt_peers)
    ]
    for copy in l1_out:
        copy.start()
    for x in xs:
        begin([image_a(my, x)])
    for y in ys:
        begin([image_b(y, mx)])

    def take_a(y):
        for x in xs:
            to_txt(
                g1a.at[x, y], g1a.at[x, y], a1_send.at[x, y], a1_recv.at[x, y],
                my * minor + x,
            ).wait_recv()
            gi[block(y, mx, 0), :] = gi[block(y, mx, 0), :] + g1a[x, y]

    def take_b(x):
        for y in ys:
            to_txt(
                g1b.at[y, x], g1b.at[y, x], b1_send.at[y, x], b1_recv.at[y, x],
                y * minor + mx,
            ).wait_recv()
            gi[block(my, x, 1), :] = gi[block(my, x, 1), :] + g1b[y, x]

    def second_leg():
        for y in ys:
            take_a(y)
            begin([to_txt(
                gi.at[block(y, mx, 0), :], g2a.at[my], a2_send.at[y], a2_recv.at[my],
                y * minor + mx,
            )])
        for x in xs:
            take_b(x)
            begin([to_txt(
                gi.at[block(my, x, 1), :], g2b.at[mx], b2_send.at[x], b2_recv.at[mx],
                my * minor + x,
            )])

    def loss_leg():
        for d, p in enumerate(txt_peers):
            to_txt(lrow.at[p], lrow.at[p], l1_send.at[d], l1_recv.at[p], p).wait_recv()
        lcol[mi] = functools.reduce(jnp.add, [lrow[k] for k in range(txt_n)])
        l2_out = [
            to_img(lcol.at[mi], lcol.at[mi], l2_send.at[d], l2_recv.at[mi], p)
            for d, p in enumerate(img_peers)
        ]
        for copy in l2_out:
            copy.start()
        if levels > 1:
            launch(1)
        return l2_out

    def onward(bp, h, up):
        @pl.when(jnp.logical_and(zp < bp, zp > 0) if up else zp > bp)
        def _():
            at, slot, copy = hop(real(bp), h, 1 - high if up else high)
            copy.wait_recv()
            gt[at, :] = gt[at, :] + slot[...]
            copy.start()

    steps = [
        ((levels - 1 - bp) * 2 + h, True, bp, h) for bp in range(2, levels) for h in range(2)
    ] + [
        (bp * 2 + h + 1.5, False, bp, h) for bp in range(levels // 2) for h in range(2)
    ]
    l2_out = None
    for key, up, bp, h in sorted(steps):
        if key > 1 and l2_out is None:
            second_leg()
            l2_out = loss_leg()
        onward(bp, h, up)
    if l2_out is None:
        second_leg()
        l2_out = loss_leg()

    take_a(my)
    take_b(mx)
    for d, p in enumerate(img_peers):
        to_img(lcol.at[p], lcol.at[p], l2_send.at[d], l2_recv.at[p], p).wait_recv()
    loss_ref[...] = (0.5 * LN2) * functools.reduce(jnp.add, [lcol[k] for k in range(img_n)])

    for way in (0, 1):
        @pl.when(mz > 0 if way else mz < levels - 1)
        def _(way=way):
            for h in range(2):
                at, slot, copy = hop(mz, h, way)
                copy.wait_recv()
                gt[at, :] = gt[at, :] + slot[...]

    gtxt_ref[...] = gt[cols_of(mi), :]
    gimg_ref[...] = gi[rows_of(mt), :]
    for y in ys:
        to_txt(
            g2a.at[y], g2a.at[y], a2_send.at[y], a2_recv.at[y], y * minor + mx
        ).wait_recv()
        gimg_ref[0:part, :] = gimg_ref[0:part, :] + g2a[y]
    for x in xs:
        to_txt(
            g2b.at[x], g2b.at[x], b2_send.at[x], b2_recv.at[x], my * minor + x
        ).wait_recv()
        gimg_ref[part:per, :] = gimg_ref[part:per, :] + g2b[x]
    for b in range(levels):
        for way in (0, 1):
            @pl.when(b > mz if way else b < mz)
            def _(b=b, way=way):
                for h in range(2):
                    hop(b, h, way)[2].wait_send()

    for copy in [*stat_out, *gi_out, *x_out, *l1_out, *l2_out]:
        copy.wait_send()


def hand_over(loss, gimg, gtxt, loss_out, gimg_out, gtxt_out, sem):
    copies = [
        pltpu.make_async_copy(gimg, gimg_out, sem.at[0]),
        pltpu.make_async_copy(gtxt, gtxt_out, sem.at[1]),
    ]
    for copy in copies:
        copy.start()
    loss_out[0, 0] = loss[0, 0]
    for copy in copies:
        copy.wait()


def body(img_n, txt_n, teacher_img, teacher_txt, student_img, student_txt):
    rows, wide = teacher_img.shape
    cols, deep = student_txt.shape
    levels = img_n // 2
    vmem = pltpu.VMEM
    minor = minor_of(txt_n)
    major = txt_n // minor
    part = rows // txt_n // 2
    dma = pltpu.SemaphoreType.DMA
    bf16 = jnp.bfloat16
    loss, grad_img, grad_txt = pl.pallas_call(
        functools.partial(kernel, img_n, txt_n),
        out_shape=(
            jax.ShapeDtypeStruct((8, LANES), F32),
            jax.ShapeDtypeStruct((rows // txt_n, deep), F32),
            jax.ShapeDtypeStruct((cols // img_n, deep), F32),
        ),
        in_specs=[pl.BlockSpec(memory_space=pltpu.HBM)] * 4,
        out_specs=tuple(pl.BlockSpec(memory_space=vmem) for _ in range(3)),
        scratch_shapes=[
            vmem((rows, wide), bf16), vmem((cols, wide), bf16),
            vmem((rows, deep), bf16), vmem((cols, deep), bf16),
            vmem((rows, cols), F32), vmem((rows, cols), F32), vmem((rows, cols), F32),
            vmem((2, rows, LANES), F32), vmem((2, rows, LANES), F32), vmem((2, 8, cols), F32),
            vmem((2, txt_n, rows // LANES, LANES), F32),
            vmem((2, img_n, cols // LANES, LANES), F32),
            vmem((txt_n, rows // txt_n, cols), bf16), vmem((levels, cols // levels, rows), bf16),
            vmem((rows, deep), F32), vmem((minor, major, part, deep), F32),
            vmem((major, minor, part, deep), F32),
            vmem((major, part, deep), F32), vmem((minor, part, deep), F32),
            vmem((cols, deep), F32), vmem((levels, cols // img_n, deep), F32),
            vmem((2, levels, cols // img_n, deep), F32),
            vmem((txt_n, 8, LANES), F32), vmem((img_n, 8, LANES), F32),
            dma((4,)),
            dma((2, txt_n)), dma((2, txt_n)), dma((2, img_n)), dma((2, img_n)),
            dma((minor, major)), dma((minor, major)), dma((major, minor)), dma((major, minor)),
            dma((major,)), dma((major,)), dma((minor,)), dma((minor,)), dma((levels,)), dma((levels,)),
            dma((2, levels, 2)), dma((2, levels, 2)),
            dma((txt_n,)), dma((txt_n,)), dma((img_n,)), dma((img_n,)),
        ],
        compiler_params=pltpu.CompilerParams(
            collective_id=0, has_side_effects=True, vmem_limit_bytes=48 * 1024 * 1024
        ),
    )(*[pltpu.with_memory_space_constraint(v, pltpu.HBM) for v in (teacher_img, teacher_txt, student_img, student_txt)])
    loss, grad_img, grad_txt = pl.pallas_call(
        hand_over,
        out_shape=(
            jax.ShapeDtypeStruct((1, 1), F32),
            jax.ShapeDtypeStruct(grad_img.shape, F32),
            jax.ShapeDtypeStruct(grad_txt.shape, F32),
        ),
        in_specs=[pl.BlockSpec(memory_space=vmem)] * 3,
        out_specs=(
            pl.BlockSpec(memory_space=pltpu.SMEM),
            pl.BlockSpec(memory_space=pltpu.HBM), pl.BlockSpec(memory_space=pltpu.HBM),
        ),
        scratch_shapes=[dma((2,))],
        compiler_params=pltpu.CompilerParams(vmem_limit_bytes=1024 * 1024),
    )(loss, grad_img, grad_txt)
    return loss.reshape(()), grad_img, grad_txt


def solution(mesh):
    placed = (P("img", None), P("txt", None), P("img", None), P("txt", None))
    return jax.shard_map(
        functools.partial(body, mesh.shape["img"], mesh.shape["txt"]),
        mesh=mesh,
        in_specs=placed,
        out_specs=(P(), P(("img", "txt"), None), P(("txt", "img"), None)),
        check_vma=False,
    )
```
